64 devices in a mesh: data: 4 (over x, y), stage: 16 (over z, core).
Axes of the slice: x: 2, y: 2, z: 8, core: 2. Of those that a mesh axis runs over, the one named last changes fastest.
The devices are a block of a 4x4x8 slice.
Arguments:
- x_init: float32 [8, 256, 16], P('data'), parts along dimension 0
- h_warm: bfloat16 [15, 8, 256, 512], P(None, 'data'), parts along dimension 1
- skip_warm: bfloat16 [8, 8, 256, 512], P(None, 'data'), parts along dimension 1
- w_in: bfloat16 [16, 512], replicated
- w_out: bfloat16 [512, 16], replicated
- w_qkv: bfloat16 [16, 512, 1536], P('stage')
- w_o: bfloat16 [16, 8, 64, 512], P('stage')
- w_up: bfloat16 [16, 512, 2048], P('stage')
- w_down: bfloat16 [16, 2048, 512], P('stage')
- w_skip: bfloat16 [8, 1024, 512], replicated
- ada_mods: float32 [32, 16, 6, 512], P(None, 'stage')
- coef_keep: float32 [32], replicated
- coef_noise: float32 [32], replicated
Outputs:
- output: float32 [8, 256, 16], P('data'), parts along dimension 0
There are 4 independent parts. The reference program is written for one: setup_inputs(seed, part) draws one part's arguments, and reference() takes and returns one part's arrays. A program takes and returns all parts, laid end to end along the dimension named above; an argument that names none is the same for every part.
All inputs are finite; a program needn't handle non-finite values.
Results may differ from the reference program's by a relative error of at most 0.0126811.
Values are sent between devices in bfloat16 or wider.
A program may use at most 768 MiB of HBM per device.

```python
import jax
import jax.numpy as jnp
from jax import lax
import math

WIDTH = 512
NUM_HEADS = 8
LAYERS = 16
TOKENS = 256
CHANNELS = 16
STAGES = 16
BATCH_PART = 2
NUM_STEPS = 32

HEAD_DIM = WIDTH // NUM_HEADS
PER_STAGE = LAYERS // STAGES
HALF_LAYERS = LAYERS // 2
HALF_STAGES = STAGES // 2
N_ROWS = BATCH_PART * TOKENS
SCORE_SCALE = 1.0 / math.sqrt(HEAD_DIM)
LN_EPS = 1e-6


def setup_inputs(seed: int = 0, part: int = 0) -> dict:
    base_key = jax.random.key(seed)
    weight_keys = jax.random.split(base_key, 10)
    part_keys = jax.random.split(jax.random.fold_in(base_key, part), 3)

    def weight(key_one, array_shape, fan_in):
        return (jax.random.normal(key_one, array_shape, jnp.float32) / math.sqrt(fan_in)).astype(jnp.bfloat16)

    x_init = jax.random.normal(part_keys[0], (BATCH_PART, TOKENS, CHANNELS), jnp.float32)
    h_warm = jax.random.normal(part_keys[1], (STAGES - 1, BATCH_PART, TOKENS, WIDTH), jnp.float32).astype(jnp.bfloat16)
    skip_warm = jax.random.normal(part_keys[2], (HALF_LAYERS, BATCH_PART, TOKENS, WIDTH), jnp.float32).astype(jnp.bfloat16)
    gate_mean = jnp.array([0.0, 0.0, 0.6, 0.0, 0.0, 0.6], dtype=jnp.float32).reshape(1, 1, 6, 1)
    ada_mods = gate_mean + 0.2 * jax.random.normal(weight_keys[7], (NUM_STEPS, LAYERS, 6, WIDTH), jnp.float32)
    return dict(
        x_init=x_init,
        h_warm=h_warm,
        skip_warm=skip_warm,
        w_in=weight(weight_keys[0], (CHANNELS, WIDTH), CHANNELS),
        w_out=weight(weight_keys[1], (WIDTH, CHANNELS), WIDTH),
        w_qkv=weight(weight_keys[2], (LAYERS, WIDTH, 3 * WIDTH), WIDTH),
        w_o=weight(weight_keys[3], (LAYERS, NUM_HEADS, HEAD_DIM, WIDTH), WIDTH),
        w_up=weight(weight_keys[4], (LAYERS, WIDTH, 4 * WIDTH), WIDTH),
        w_down=weight(weight_keys[5], (LAYERS, 4 * WIDTH, WIDTH), 4 * WIDTH),
        w_skip=weight(weight_keys[6], (HALF_LAYERS, 2 * WIDTH, WIDTH), 2 * WIDTH),
        ada_mods=ada_mods,
        coef_keep=jax.random.uniform(weight_keys[8], (NUM_STEPS,), jnp.float32, 0.7, 0.95),
        coef_noise=-jax.random.uniform(weight_keys[9], (NUM_STEPS,), jnp.float32, 0.2, 0.5),
    )


def layer_norm(hidden):
    centered = hidden - jnp.mean(hidden, axis=-1, keepdims=True)
    variance = jnp.mean(centered * centered, axis=-1, keepdims=True)
    return centered * lax.rsqrt(variance + LN_EPS)


def attention_one(qkv_one):
    queries = qkv_one[:, 0].astype(jnp.float32)
    key_rows = qkv_one[:, 1].astype(jnp.float32)
    value_rows = qkv_one[:, 2].astype(jnp.float32)
    scores = jnp.einsum('qhd,khd->hqk', queries, key_rows) * SCORE_SCALE
    attn_probs = jax.nn.softmax(scores, axis=-1).astype(jnp.bfloat16).astype(jnp.float32)
    return jnp.einsum('hqk,khd->qhd', attn_probs, value_rows).astype(jnp.bfloat16)


def dit_block(hidden, block_mod, wqkv_one, wo_one, wup_one, wdown_one):
    normed = layer_norm(hidden) * (1.0 + block_mod[1]) + block_mod[0]
    qkv_all = jnp.dot(normed.astype(jnp.bfloat16).reshape(N_ROWS, WIDTH), wqkv_one, preferred_element_type=jnp.float32).astype(jnp.bfloat16)
    attended = lax.map(attention_one, qkv_all.reshape(BATCH_PART, TOKENS, 3, NUM_HEADS, HEAD_DIM))
    attn_out = jnp.dot(attended.reshape(N_ROWS, WIDTH), wo_one.reshape(WIDTH, WIDTH), preferred_element_type=jnp.float32)
    hidden = hidden + block_mod[2] * attn_out.reshape(BATCH_PART, TOKENS, WIDTH)
    normed = layer_norm(hidden) * (1.0 + block_mod[4]) + block_mod[3]
    mlp_hidden = jnp.dot(normed.astype(jnp.bfloat16).reshape(N_ROWS, WIDTH), wup_one, preferred_element_type=jnp.float32)
    gelu_act = jax.nn.gelu(mlp_hidden, approximate=True).astype(jnp.bfloat16)
    mlp_out = jnp.dot(gelu_act, wdown_one, preferred_element_type=jnp.float32)
    return hidden + block_mod[5] * mlp_out.reshape(BATCH_PART, TOKENS, WIDTH)


def skip_project(hidden, skip_one, wskip_one):
    main_part = jnp.dot(hidden.astype(jnp.bfloat16).reshape(N_ROWS, WIDTH), wskip_one[:WIDTH], preferred_element_type=jnp.float32)
    skip_part = jnp.dot(skip_one.reshape(N_ROWS, WIDTH), wskip_one[WIDTH:], preferred_element_type=jnp.float32)
    return (main_part + skip_part).reshape(BATCH_PART, TOKENS, WIDTH)


def reference(x_init, h_warm, skip_warm, w_in, w_out, w_qkv, w_o, w_up, w_down, w_skip, ada_mods, coef_keep, coef_noise):
    def run_stage(stage_in, stage_id, step_mods, skip_in):
        skip_for = jnp.flip(skip_in, 0)

        def layer_body(hidden, offset):
            block_id = stage_id * PER_STAGE + offset
            skip_id = jnp.maximum(block_id - HALF_LAYERS, 0)
            projected = skip_project(hidden, skip_for[skip_id], w_skip[skip_id])
            hidden = jnp.where(block_id >= HALF_LAYERS, projected, hidden)
            hidden = dit_block(hidden, step_mods[block_id], w_qkv[block_id], w_o[block_id], w_up[block_id], w_down[block_id])
            return hidden, hidden.astype(jnp.bfloat16)

        return lax.scan(layer_body, stage_in, jnp.arange(PER_STAGE))[1]

    def step_body(state_in, step_in):
        latent, bound_in, skip_in = state_in
        step_mods, keep_one, noise_one = step_in
        from_latent = jnp.dot(latent.astype(jnp.bfloat16).reshape(N_ROWS, CHANNELS), w_in, preferred_element_type=jnp.float32).reshape(BATCH_PART, TOKENS, WIDTH)
        stage_ins = jnp.concatenate([from_latent[None], bound_in.astype(jnp.float32)], axis=0)

        def stage_fn(stage_pair):
            return run_stage(stage_pair[0], stage_pair[1], step_mods, skip_in)

        block_outs = lax.map(stage_fn, (stage_ins, jnp.arange(STAGES)))
        last_out = block_outs[STAGES - 1, PER_STAGE - 1]
        noise_pred = jnp.dot(last_out.reshape(N_ROWS, WIDTH), w_out, preferred_element_type=jnp.float32).reshape(BATCH_PART, TOKENS, CHANNELS)
        new_latent = keep_one * latent + noise_one * noise_pred
        new_bound = block_outs[:STAGES - 1, PER_STAGE - 1]
        new_skips = block_outs[:HALF_STAGES].reshape(HALF_LAYERS, BATCH_PART, TOKENS, WIDTH)
        return (new_latent, new_bound, new_skips), None

    final_state = lax.scan(step_body, (x_init, h_warm, skip_warm), (ada_mods, coef_keep, coef_noise))[0]
    return final_state[0]
```

```python
import functools
import math

import jax
import jax.numpy as jnp
from jax import lax
from jax.experimental import pallas as pl
from jax.experimental.pallas import tpu as pltpu
from jax.sharding import PartitionSpec as P

F32 = jnp.float32
BF16 = jnp.bfloat16
PIECE = 64
CHUNK = 256
NP = CHUNK // PIECE
CORES = 2
SLOTS = 4
EPS = 1e-6
LAG = 4
TANH_A = math.sqrt(2.0 / math.pi)
TANH_B = TANH_A * 0.044715


class Unit:
    def __init__(self):
        self.accs, self.next, self.rhs = {}, 0, None

    def alloc(self, count):
        ids = list(range(self.next, self.next + count))
        self.next += count
        return ids

    def push(self, rhs):
        self.rhs = rhs
        return 0

    def feed(self, reg, ids, lhs):
        for n, a in enumerate(ids):
            v = jnp.dot(lhs(n), self.rhs, preferred_element_type=F32)
            self.accs[a] = self.accs[a] + v if a in self.accs else v

    def pop(self, a):
        return self.accs.pop(a)


def accumulators():
    return []


def make_units(accs):
    return [Unit(), Unit()]


def norm_mod(h, scale, shift):
    width = h.shape[0]
    mean = jnp.sum(h, axis=0, keepdims=True) * (1.0 / width)
    c = h - mean
    var = jnp.sum(c * c, axis=0, keepdims=True) * (1.0 / width)
    return ((c * lax.rsqrt(var + EPS)) * scale + shift).astype(BF16)


def gelu(x):
    return (x * (0.5 + 0.5 * jnp.tanh(x * (TANH_A + TANH_B * (x * x))))).astype(BF16)


def softmax(s, scale):
    m = jnp.max(s, axis=0, keepdims=True)
    p = jnp.exp2((s - m) * (scale * math.log2(math.e)))
    return (p * (1.0 / jnp.sum(p, axis=0, keepdims=True))).astype(BF16)


def wide(cols):
    return jnp.concatenate([cols, cols], axis=1)


def spread(mods, dst):
    cols = mods.T
    for v in range(6):
        col = cols[:, v : v + 1]
        if v in (1, 4):
            col = 1.0 + col
        dst[v] = jnp.broadcast_to(col, dst.shape[1:])


def block(units, h_ref, mod, w_qkv, w_o, w_up, w_down, out, t, heads, extra):
    width, tokens = h_ref.shape
    ff = w_up.shape[0]
    dim = width // heads
    ktiles = width // CHUNK
    per_group = CHUNK // dim
    groups = heads // per_group

    def project(q, w, row, rhs, nk, done):
        u = units[q]
        ids = u.alloc(NP)
        for k in range(nk):
            reg = u.push(rhs(k))
            u.feed(reg, ids, lambda n: w[row + PIECE * n : row + PIECE * (n + 1), CHUNK * k : CHUNK * (k + 1)])
        for n, a in enumerate(ids):
            done(row + PIECE * n, u.pop(a))

    def u_tile(k):
        return t.u[CHUNK * k : CHUNK * (k + 1), :]

    t.u[...] = norm_mod(h_ref[...], wide(mod[1]), wide(mod[0]))

    def keep_qkv(row, v):
        t.qkv[row : row + PIECE, :] = v.astype(BF16)

    for part in (1, 0, 2):
        for g in range(groups):
            project(g % 2, w_qkv, width * part + CHUNK * g, u_tile, ktiles, keep_qkv)

    zero = jnp.zeros((dim, tokens), BF16)
    keys = [t.qkv[width + CHUNK * g : width + CHUNK * (g + 1), :].T for g in range(groups)]

    def scores(hd):
        g, j = divmod(hd, per_group)
        query = t.qkv[dim * hd : dim * (hd + 1), :]
        padded = jnp.concatenate([query if n == j else zero for n in range(per_group)], axis=0)
        u = units[g % 2]
        ids = u.alloc(NP)
        reg = u.push(padded)
        u.feed(reg, ids, lambda n: keys[g][PIECE * n : PIECE * (n + 1)])
        for n, a in enumerate(ids):
            t.s[g, j % 2, PIECE * n : PIECE * (n + 1), :] = u.pop(a)

    def probs(hd):
        g, j = divmod(hd, per_group)
        for c in range(0, tokens, 128):
            t.p[g, j % 2, :, c : c + 128] = softmax(t.s[g, j % 2, :, c : c + 128], 1.0 / math.sqrt(dim))

    def values(hd):
        g, j = divmod(hd, per_group)
        u = units[g % 2]
        reg = u.push(t.p[g, j % 2])
        ids = u.alloc(1)
        u.feed(reg, ids, lambda n: t.qkv[2 * width + dim * hd : 2 * width + dim * (hd + 1), :])
        t.o[dim * hd : dim * (hd + 1), :] = u.pop(ids[0]).astype(BF16)

    for g in range(groups):
        scores(g * per_group)
    for j in range(per_group):
        for g in range(groups):
            hd = g * per_group + j
            if j + 1 < per_group:
                scores(hd + 1)
            probs(hd)
            values(hd)

    def o_tile(k):
        return t.o[CHUNK * k : CHUNK * (k + 1), :]

    def add_attn(row, v):
        h_ref[row : row + PIECE, :] = h_ref[row : row + PIECE, :] + wide(mod[2, row : row + PIECE]) * v

    for n in range(width // CHUNK):
        project(n % 2, w_o, CHUNK * n, o_tile, ktiles, add_attn)

    t.u[...] = norm_mod(h_ref[...], wide(mod[4]), wide(mod[3]))
    down_ids = [u.alloc(NP) for u in units]
    chunks = ff // CHUNK

    def up(n):
        u = units[n % 2]
        ids = u.alloc(NP)
        for k in range(ktiles):
            reg = u.push(u_tile(k))
            u.feed(
                reg,
                ids,
                lambda m: w_up[CHUNK * n + PIECE * m : CHUNK * n + PIECE * (m + 1), CHUNK * k : CHUNK * (k + 1)],
            )
        return ids

    def down(k):
        for q, u in enumerate(units):
            reg = u.push(t.act[CHUNK * k : CHUNK * (k + 1), :])
            u.feed(
                reg,
                down_ids[q],
                lambda m: w_down[CHUNK * q + PIECE * m : CHUNK * q + PIECE * (m + 1), CHUNK * k : CHUNK * (k + 1)],
            )

    for n in range(chunks):
        ids = up(n)
        if n >= LAG:
            down(n - LAG)
        for m, a in enumerate(ids):
            t.act[CHUNK * n + PIECE * m : CHUNK * n + PIECE * (m + 1), :] = gelu(units[n % 2].pop(a))
        if n == 0:
            extra()
    for n in range(chunks - LAG, chunks):
        down(n)
    for q, u in enumerate(units):
        for m, a in enumerate(down_ids[q]):
            row = CHUNK * q + PIECE * m
            h = h_ref[row : row + PIECE, :] + wide(mod[5, row : row + PIECE]) * u.pop(a)
            out[row : row + PIECE, :] = h.astype(BF16)


class Scratch:
    pass


def solution(mesh):
    stages = mesh.shape["stage"]
    chips = stages // CORES

    def kernel(
        steps, heads,
        x_ref, hwarm_ref, swarm_ref, win_ref, wout_ref, wqkv_ref, wo_ref, wup_ref, wdown_ref, wskip_ref, mods_ref,
        keep_ref, noise_ref,
        out_ref,
        raw_qkv, raw_o, raw_up, raw_down, stg_qkv, stg_o, stg_up, stg_down, stg_mod,
        w_qkv, w_o, w_up, w_down, w_mod, raw_skip, w_skip, raw_warm, w_in, w_out,
        in_a, in_b, out_a, out_b, x_t, x_all, h_ref, s_u, s_qkv, s_o, s_act, s_s, s_p, mod_a, mod_b,
        load_sem, warm_sem, wsend_sem, wrecv_sem, fsend_sem, frecv_sem,
        asend_sem, arecv_sem, bsend_sem, brecv_sem, xsend_sem, xrecv_sem,
    ):
        me = lax.axis_index("stage")
        chip, core = me // CORES, lax.rem(me, CORES)
        pair = lax.rem(chips - chip, chips)
        sample = lax.rem(core + pair, CORES)
        last_pair = chips - 1

        def device(chip_, core_):
            return {"stage": chip_ * CORES + core_}

        raws = [raw_qkv, raw_o, raw_up, raw_down]
        homes = [wqkv_ref, wo_ref, wup_ref, wdown_ref]
        loads = [pltpu.make_async_copy(src.at[0], dst, load_sem.at[n]) for n, (src, dst) in enumerate(zip(homes, raws))]
        loads.append(pltpu.make_async_copy(mods_ref.at[:, 0], stg_mod, load_sem.at[4]))
        loads.append(pltpu.make_async_copy(wskip_ref.at[last_pair - pair], raw_skip, load_sem.at[5]))
        warm = [
            pltpu.make_async_copy(hwarm_ref.at[jnp.maximum(pair - 1, 0), sample], raw_warm.at[0], warm_sem.at[0]),
            pltpu.make_async_copy(hwarm_ref.at[stages - 2 - pair, sample], raw_warm.at[1], warm_sem.at[1]),
            pltpu.make_async_copy(swarm_ref.at[pair, sample], raw_warm.at[2], warm_sem.at[2]),
        ]
        for copy in loads + warm:
            copy.start()

        home_pair = jnp.minimum(me, stages - 1 - me)
        home_slot = jnp.where(me < chips, 0, 1)
        goal = lax.rem(chips - home_pair, chips)

        def turn(src, dst):
            cols = src.shape[1]

            def body(n, _):
                at = pl.multiple_of(n * CHUNK, CHUNK)
                dst[pl.ds(at, CHUNK), :] = src[:, pl.ds(at, CHUNK)].T
                return 0

            lax.fori_loop(0, cols // CHUNK, body, 0)

        stages_of = [stg_qkv, stg_o, stg_up, stg_down, stg_mod]
        slots_of = [w_qkv, w_o, w_up, w_down, w_mod]

        def part(n, slot, cc):
            half = slots_of[n].shape[1] // CORES
            return slots_of[n].at[slot, pl.ds(pl.multiple_of(cc * half, half), half)]

        def home_part(n, cc):
            half = stages_of[n].shape[0] // CORES
            return stages_of[n].at[pl.ds(cc * half, half)]

        def direct(n, cc):
            return pltpu.make_async_remote_copy(
                src_ref=home_part(n, cc),
                dst_ref=part(n, home_slot, cc),
                send_sem=wsend_sem.at[n, cc],
                recv_sem=wrecv_sem.at[home_slot, n],
                device_id=device(goal, cc),
                device_id_type=pl.DeviceIdType.MESH,
            )

        def stay(n, cc):
            return pltpu.make_async_copy(home_part(n, cc), part(n, home_slot, cc), wrecv_sem.at[home_slot, n])

        def forward(n, slot):
            return pltpu.make_async_remote_copy(
                src_ref=part(n, slot, core),
                dst_ref=part(n, slot, core),
                send_sem=fsend_sem.at[slot, n],
                recv_sem=frecv_sem.at[slot, n],
                device_id=device(chip, 1 - core),
                device_id_type=pl.DeviceIdType.MESH,
            )

        for n in range(5):
            loads[n].wait()
            if n < 4:
                turn(raws[n], stages_of[n])
            for cc in range(CORES):
                mine = goal * CORES + cc == me

                @pl.when(mine)
                def _():
                    stay(n, cc).start()

                @pl.when(jnp.logical_not(mine))
                def _():
                    direct(n, cc).start()

        loads[5].wait()
        turn(raw_skip.at[0 : raw_skip.shape[1]], w_skip.at[0])
        turn(raw_skip.at[raw_skip.shape[1] :], w_skip.at[1])
        for copy in warm:
            copy.wait()
        in_a[0] = raw_warm[0].T
        in_b[0] = raw_warm[1].T
        out_a[1] = raw_warm[2].T
        x_t[...] = x_ref[sample].T
        w_in[...] = jnp.zeros_like(w_in)
        w_in[:, 0 : win_ref.shape[0]] = win_ref[...].T
        w_out[...] = wout_ref[...].T

        for slot in range(2):
            for n in range(5):
                pltpu.make_async_copy(part(n, slot, core), part(n, slot, core), wrecv_sem.at[slot, n]).wait()
                forward(n, slot).start()
        for slot in range(2):
            for n in range(5):
                forward(n, slot).wait_recv()

        t = Scratch()
        t.u, t.qkv, t.o, t.act, t.s, t.p = s_u, s_qkv, s_o, s_act, s_s, s_p
        channels = x_ref.shape[2]

        def a_copy(k):
            return pltpu.make_async_remote_copy(
                src_ref=out_a.at[lax.rem(k, 2)],
                dst_ref=in_a.at[lax.rem(k + 1, SLOTS)],
                send_sem=asend_sem.at[lax.rem(k, 2)],
                recv_sem=arecv_sem.at[lax.rem(k + 1, SLOTS)],
                device_id=device(lax.rem(chip + chips - 1, chips), 1 - core),
                device_id_type=pl.DeviceIdType.MESH,
            )

        def a_stay(k):
            return pltpu.make_async_copy(
                out_a.at[lax.rem(k, 2)], in_b.at[lax.rem(k + 1, SLOTS)], brecv_sem.at[lax.rem(k + 1, SLOTS)]
            )

        def b_copy(k):
            return pltpu.make_async_remote_copy(
                src_ref=out_b.at[lax.rem(k, 2)],
                dst_ref=in_b.at[lax.rem(k + 1, SLOTS)],
                send_sem=bsend_sem.at[lax.rem(k, 2)],
                recv_sem=brecv_sem.at[lax.rem(k + 1, SLOTS)],
                device_id=device(lax.rem(chip + 1, chips), 1 - core),
                device_id_type=pl.DeviceIdType.MESH,
            )

        def landed(buf, sem, k):
            slot = lax.rem(k, SLOTS)
            pltpu.make_async_copy(buf.at[slot], buf.at[slot], sem.at[slot]).wait()

        def compute(*accs):
            units = make_units(accs)

            spread(w_mod[0, 0], mod_a)

            def step(k, _):
                slot = lax.rem(k, SLOTS)
                here, before = lax.rem(k, 2), lax.rem(k + 1, 2)

                @pl.when(k < steps - 1 - pair)
                def _():
                    @pl.when(pair == 0)
                    def _():
                        x_pad = jnp.concatenate(
                            [x_t[...].astype(BF16), jnp.zeros((CHUNK - channels, x_t.shape[1]), BF16)], axis=0
                        )
                        for q, u in enumerate(units):
                            ids = u.alloc(NP)
                            reg = u.push(x_pad)
                            u.feed(reg, ids, lambda n: w_in[CHUNK * q + PIECE * n : CHUNK * q + PIECE * (n + 1), :])
                            for n, a in enumerate(ids):
                                h_ref[CHUNK * q + PIECE * n : CHUNK * q + PIECE * (n + 1), :] = u.pop(a)

                    @pl.when(pair > 0)
                    def _():
                        @pl.when(k > 0)
                        def _():
                            landed(in_a, arecv_sem, k)

                        h_ref[...] = in_a[slot].astype(F32)

                    @pl.when(jnp.logical_and(k > 1, pair < last_pair))
                    def _():
                        a_copy(k - 2).wait_send()

                    block(
                        units, h_ref, mod_a, w_qkv.at[0], w_o.at[0], w_up.at[0], w_down.at[0], out_a.at[here], t, heads,
                        lambda: spread(w_mod[1, k], mod_b),
                    )

                    @pl.when(pair == last_pair)
                    def _():
                        a_stay(k).start()

                    @pl.when(jnp.logical_and(pair < last_pair, k < steps - 3 - pair))
                    def _():
                        a_copy(k).start()

                @pl.when(k == steps - 1 - pair)
                def _():
                    spread(w_mod[1, k], mod_b)

                @pl.when(k > 0)
                def _():
                    landed(in_b, brecv_sem, k)

                @pl.when(jnp.logical_and(k > 1, pair > 0))
                def _():
                    b_copy(k - 2).wait_send()

                for q, u in enumerate(units):
                    ids = u.alloc(NP)
                    for half in range(2):
                        for n in range(h_ref.shape[0] // CHUNK):
                            rows = slice(CHUNK * n, CHUNK * (n + 1))
                            reg = u.push(in_b[slot, rows, :] if half == 0 else out_a[before, rows, :])
                            u.feed(
                                reg,
                                ids,
                                lambda m: w_skip[half, CHUNK * q + PIECE * m : CHUNK * q + PIECE * (m + 1), rows],
                            )
                    for m, a in enumerate(ids):
                        h_ref[CHUNK * q + PIECE * m : CHUNK * q + PIECE * (m + 1), :] = u.pop(a)
                block(
                    units, h_ref, mod_b, w_qkv.at[1], w_o.at[1], w_up.at[1], w_down.at[1], out_b.at[here], t, heads,
                    lambda: spread(w_mod[0, jnp.minimum(k + 1, steps - 1)], mod_a),
                )

                @pl.when(pair > 0)
                def _():
                    b_copy(k).start()

                @pl.when(pair == 0)
                def _():
                    u = units[0]
                    [a] = u.alloc(1)
                    pad = jnp.zeros((PIECE - channels, CHUNK), BF16)
                    for n in range(h_ref.shape[0] // CHUNK):
                        rows = slice(CHUNK * n, CHUNK * (n + 1))
                        reg = u.push(out_b[here, rows, :])
                        u.feed(reg, [a], lambda _: jnp.concatenate([w_out[:, rows], pad], axis=0))
                    noise = u.pop(a)[0:channels, :]
                    x_t[...] = keep_ref[k] * x_t[...] + noise_ref[k] * noise

                return 0

            lax.fori_loop(0, steps - pair, step, 0)

        compute()

        count = steps - pair

        @pl.when(pair > 0)
        def _():
            b_copy(count - 2).wait_send()
            b_copy(count - 1).wait_send()

        for n in range(5):
            for cc in range(CORES):

                @pl.when(goal * CORES + cc != me)
                def _():
                    direct(n, cc).wait_send()

            for slot in range(2):
                forward(n, slot).wait_send()

        def share(n, who):
            return pltpu.make_async_remote_copy(
                src_ref=x_t,
                dst_ref=x_all.at[who],
                send_sem=xsend_sem.at[n],
                recv_sem=xrecv_sem.at[who],
                device_id={"stage": n},
                device_id_type=pl.DeviceIdType.MESH,
            )

        @pl.when(pair == 0)
        def _():
            for n in range(stages):

                @pl.when(n != me)
                def _():
                    share(n, sample).start()

            own = pltpu.make_async_copy(x_t, x_all.at[sample], xrecv_sem.at[sample])
            own.start()
            for n in range(stages):

                @pl.when(n != me)
                def _():
                    share(n, sample).wait_send()

        for n in range(CORES):
            pltpu.make_async_copy(x_t, x_all.at[n], xrecv_sem.at[n]).wait()
            out_ref[n] = x_all[n].T

    def local_run(x_init, h_warm, skip_warm, w_in, w_out, w_qkv, w_o, w_up, w_down, w_skip, ada_mods, keep, noise):
        batch, tokens, channels = x_init.shape
        width, ff = w_up.shape[1], w_up.shape[2]
        heads = w_o.shape[1]
        steps = ada_mods.shape[0]
        any_ = pl.BlockSpec(memory_space=pl.ANY)
        vmem = pl.BlockSpec(memory_space=pltpu.VMEM)
        smem = pl.BlockSpec(memory_space=pltpu.SMEM)
        V = pltpu.VMEM
        D = pltpu.SemaphoreType.DMA
        scratch = [
            V((width, 3 * width), BF16), V((width, width), BF16), V((width, ff), BF16), V((ff, width), BF16),
            V((3 * width, width), BF16), V((width, width), BF16), V((ff, width), BF16), V((width, ff), BF16),
            V((steps, 6, width), F32),
            V((2, 3 * width, width), BF16), V((2, width, width), BF16), V((2, ff, width), BF16), V((2, width, ff), BF16),
            V((2, steps, 6, width), F32),
            V((2 * width, width), BF16), V((2, width, width), BF16), V((3, tokens, width), BF16),
            V((width, CHUNK), BF16), V((channels, width), BF16),
            V((SLOTS, width, tokens), BF16), V((SLOTS, width, tokens), BF16),
            V((2, width, tokens), BF16), V((2, width, tokens), BF16),
            V((channels, tokens), F32), V((CORES, channels, tokens), F32), V((width, tokens), F32),
            V((width, tokens), BF16), V((3 * width, tokens), BF16), V((width, tokens), BF16), V((ff, tokens), BF16),
            V((2, 2, tokens, tokens), F32), V((2, 2, tokens, tokens), BF16),
            V((6, width, 128), F32), V((6, width, 128), F32),
            D((6,)), D((3,)), D((5, CORES)), D((2, 5)), D((2, 5)), D((2, 5)),
            D((2,)), D((SLOTS,)), D((2,)), D((SLOTS,)), D((stages,)), D((CORES,)),
        ]
        call = pl.pallas_call(
            functools.partial(kernel, steps, heads),
            out_shape=jax.ShapeDtypeStruct((batch, tokens, channels), F32),
            in_specs=[vmem, any_, any_, vmem, vmem, any_, any_, any_, any_, any_, any_, smem, smem],
            out_specs=vmem,
            scratch_shapes=scratch,
            compiler_params=pltpu.CompilerParams(has_side_effects=True, vmem_limit_bytes=60 * 2**20),
            name="staged_sampler",
        )
        return call(
            x_init, h_warm, skip_warm, w_in, w_out, w_qkv, w_o.reshape(1, width, width), w_up, w_down, w_skip, ada_mods,
            keep, noise,
        )

    in_specs = (P('data'), P(None, 'data'), P(None, 'data'), P(), P(), P('stage'), P('stage'), P('stage'), P('stage'), P(), P(None, 'stage'), P(), P())
    return jax.shard_map(local_run, mesh=mesh, in_specs=in_specs, out_specs=P('data'), check_vma=False)
```

```python
import functools
import math

import jax
import jax.numpy as jnp
from jax import lax
from jax.experimental import pallas as pl
from jax.experimental.pallas import tpu as pltpu
from jax.sharding import PartitionSpec as P

F32 = jnp.float32
BF16 = jnp.bfloat16
CHUNK = 256
CORES = 2
COLUMNS = 4
SHARES = CORES * COLUMNS
PIECES = 3
SLOTS = 4
EPS = 1e-6
TANH_A = math.sqrt(2.0 / math.pi)
TANH_B = TANH_A * 0.044715


def product(lhs, rhs):
    return jnp.dot(lhs, rhs, preferred_element_type=F32)


def norm_mod(h, scale, shift):
    width = h.shape[0]
    mean = jnp.sum(h, axis=0, keepdims=True) * (1.0 / width)
    c = h - mean
    var = jnp.sum(c * c, axis=0, keepdims=True) * (1.0 / width)
    return ((c * lax.rsqrt(var + EPS)) * scale + shift).astype(BF16)


def gelu(x):
    return (x * (0.5 + 0.5 * jnp.tanh(x * (TANH_A + TANH_B * (x * x))))).astype(BF16)


def softmax(s, scale):
    m = jnp.max(s, axis=0, keepdims=True)
    p = jnp.exp2((s - m) * (scale * math.log2(math.e)))
    return (p * (1.0 / jnp.sum(p, axis=0, keepdims=True))).astype(BF16)


def wide(cols):
    return jnp.concatenate([cols, cols], axis=1)


def spread(mods, dst):
    cols = mods.T
    for v in range(6):
        col = cols[:, v : v + 1]
        if v in (1, 4):
            col = 1.0 + col
        dst[v] = jnp.broadcast_to(col, dst.shape[1:])


def block(h_ref, mod, w, out, t, heads, extra):
    width, tokens = h_ref.shape
    dim = width // heads
    per_group = CHUNK // dim
    groups = heads // per_group
    row_o, row_up = 3 * width, 4 * width
    ff = (w.shape[0] - row_up) // 2
    row_down = row_up + ff

    u = norm_mod(h_ref[...], wide(mod[1]), wide(mod[0]))
    t.qkv[...] = product(w[0:row_o], u).astype(BF16)

    zero = jnp.zeros((dim, tokens), BF16)
    keys = [t.qkv[width + CHUNK * g : width + CHUNK * (g + 1), :].T for g in range(groups)]
    order = [g * per_group + j for j in range(per_group) for g in range(groups)]

    def scores(n):
        g, j = divmod(order[n], per_group)
        query = t.qkv[dim * order[n] : dim * (order[n] + 1), :]
        padded = jnp.concatenate([query if m == j else zero for m in range(per_group)], axis=0)
        t.s[n % 2] = product(keys[g], padded)

    def probs(n):
        for c in range(0, tokens, 128):
            t.p[n % 2, :, c : c + 128] = softmax(t.s[n % 2, :, c : c + 128], 1.0 / math.sqrt(dim))

    def values(n):
        row = dim * order[n]
        t.o[row : row + dim, :] = product(t.qkv[2 * width + row : 2 * width + row + dim, :], t.p[n % 2]).astype(BF16)

    scores(0)
    for n in range(heads):
        if n + 1 < heads:
            scores(n + 1)
        probs(n)
        values(n)

    h_ref[...] = h_ref[...] + wide(mod[2]) * product(w[row_o:row_up], t.o[...])
    u = norm_mod(h_ref[...], wide(mod[4]), wide(mod[3]))
    chunks = ff // width

    def up(n):
        return product(w[row_up + width * n : row_up + width * (n + 1)], u)

    held, total = up(0), None
    for n in range(chunks):
        ahead = up(n + 1) if n + 1 < chunks else None
        t.act[width * n : width * (n + 1), :] = gelu(held)
        held = ahead
        if n == 0:
            extra()
        part = product(w[row_down + width * n : row_down + width * (n + 1)], t.act[width * n : width * (n + 1), :])
        total = part if total is None else total + part
    out[...] = (h_ref[...] + wide(mod[5]) * total).astype(BF16)


class Scratch:
    pass


def solution(mesh):
    stages = mesh.shape["stage"]
    chips = stages // CORES
    side = math.isqrt(mesh.shape["data"])
    if side * side != mesh.shape["data"] or side % 2:
        raise ValueError("data axis")

    def kernel(
        steps, heads,
        x_ref, hwarm_ref, swarm_ref, win_ref, wout_ref, wqkv_ref, wo_ref, wup_ref, wdown_ref, wskip_ref, mods_ref,
        keep_ref, noise_ref,
        out_ref,
        raw_qkv, raw_o, raw_up, raw_down, home_w, home_mod, all_w, all_mod,
        raw_skip, w_skip, raw_warm, w_in, w_out,
        in_a, in_b, out_a, out_b, x_t, x_all, h_ref, s_qkv, s_o, s_act, s_s, s_p, mod_a, mod_b,
        load_sem, warm_sem, hsend_sem, get_sem, send_sem, put_sem, peer_sem,
        asend_sem, arecv_sem, bsend_sem, brecv_sem, xsend_sem, xrecv_sem,
    ):
        me = lax.axis_index("stage")
        group = lax.axis_index("data")
        chip, core = me // CORES, lax.rem(me, CORES)
        pair = lax.rem(chips - chip, chips)
        sample = lax.rem(core + pair, CORES)
        last_pair = chips - 1
        width = raw_o.shape[0]
        n_parts = PIECES + 1

        odd_x, odd_y = lax.rem(group // side, 2), lax.rem(group, 2)
        column = 2 * odd_x + odd_y
        next_x = {"data": group + side * (1 - 2 * odd_x), "stage": me}
        next_y = {"data": group + 1 - 2 * odd_y, "stage": me}
        peer = {"data": group, "stage": chip * CORES + 1 - core}
        beside_x, beside_y = 2 * (1 - odd_x) + odd_y, 2 * odd_x + 1 - odd_y
        across = 2 * (1 - odd_x) + 1 - odd_y

        def remote(src, dst, send, recv, to):
            return pltpu.make_async_remote_copy(
                src_ref=src, dst_ref=dst, send_sem=send, recv_sem=recv, device_id=to, device_id_type=pl.DeviceIdType.MESH
            )

        def arrived(ref, sem):
            pltpu.make_async_copy(ref, ref, sem).wait()

        raws = [raw_qkv, raw_o, raw_up, raw_down]
        homes = [wqkv_ref, wo_ref, wup_ref, wdown_ref]
        loads = [pltpu.make_async_copy(src.at[0], dst, load_sem.at[n]) for n, (src, dst) in enumerate(zip(homes, raws))]
        loads.append(pltpu.make_async_copy(mods_ref.at[:, 0], home_mod, load_sem.at[4]))
        loads.append(pltpu.make_async_copy(wskip_ref.at[last_pair - pair], raw_skip, load_sem.at[5]))
        warm = [
            pltpu.make_async_copy(hwarm_ref.at[jnp.maximum(pair - 1, 0), sample], raw_warm.at[0], warm_sem.at[0]),
            pltpu.make_async_copy(hwarm_ref.at[stages - 2 - pair, sample], raw_warm.at[1], warm_sem.at[1]),
            pltpu.make_async_copy(swarm_ref.at[pair, sample], raw_warm.at[2], warm_sem.at[2]),
        ]
        for n in (4, 0, 1, 2, 3, 5):
            loads[n].start()
        for copy in warm:
            copy.start()

        def turn(src, dst, row):
            def body(n, _):
                at = pl.multiple_of(n * CHUNK, CHUNK)
                dst[pl.ds(row + at, CHUNK), :] = src[:, pl.ds(at, CHUNK)].T
                return 0

            lax.fori_loop(0, src.shape[1] // CHUNK, body, 0)

        home_pair = jnp.minimum(me, stages - 1 - me)
        home_slot = jnp.where(me < chips, 0, 1)
        goal = lax.rem(chips - home_pair, chips)

        piece = home_w.shape[0] // PIECES
        share = piece // SHARES
        mod_share = steps // SHARES

        def whole(n, slot=None):
            if n == 0:
                return home_mod if slot is None else all_mod.at[slot]
            rows = pl.ds((n - 1) * piece, piece)
            return home_w.at[rows] if slot is None else all_w.at[slot, rows]

        def part(n, core_, column_, slot=None, half=None):
            at, size = core_ * COLUMNS + column_, mod_share if n == 0 else share
            at = at * size
            if half is not None:
                size //= 2
                at = at + half * size
            if n == 0:
                return home_mod.at[pl.ds(at, size)] if slot is None else all_mod.at[slot, pl.ds(at, size)]
            rows = pl.ds(pl.multiple_of((n - 1) * piece + at, 16), size)
            return home_w.at[rows] if slot is None else all_w.at[slot, rows]

        def leave(n, to_core):
            return remote(
                part(n, to_core, column), part(n, to_core, column, home_slot), hsend_sem.at[n, to_core],
                get_sem.at[home_slot, n], {"data": group, "stage": goal * CORES + to_core},
            )

        def stay(n):
            return pltpu.make_async_copy(whole(n), whole(n, home_slot), get_sem.at[home_slot, n])

        def hand(n):
            return remote(whole(n), whole(n, home_slot), hsend_sem.at[n, 0], get_sem.at[home_slot, n], peer)

        def send_home(n):
            @pl.when(goal == chip)
            def _():
                stay(n).start()
                hand(n).start()

            @pl.when(goal != chip)
            def _():
                for to_core in range(CORES):
                    leave(n, to_core).start()

        loads[4].wait()
        send_home(0)
        loads[0].wait()
        turn(raw_qkv, home_w, 0)
        loads[1].wait()
        turn(raw_o, home_w, 3 * width)
        send_home(1)
        loads[2].wait()
        turn(raw_up, home_w, 4 * width)
        send_home(2)
        loads[3].wait()
        for n in range(raw_down.shape[0] // width):
            turn(raw_down.at[width * n : width * (n + 1)], home_w, 4 * width + raw_up.shape[1] + width * n)
        send_home(3)

        loads[5].wait()
        turn(raw_skip.at[0:width], w_skip.at[0], 0)
        turn(raw_skip.at[width : 2 * width], w_skip.at[1], 0)
        for copy in warm:
            copy.wait()
        in_a[0] = raw_warm[0].T
        in_b[0] = raw_warm[1].T
        out_a[1] = raw_warm[2].T
        x_t[...] = x_ref[sample].T
        w_in[...] = jnp.zeros_like(w_in)
        w_in[:, 0 : win_ref.shape[0]] = win_ref[...].T
        w_out[...] = wout_ref[...].T

        def gather(slot):
            def to_x(n):
                ref = part(n, core, column, slot)
                return remote(ref, ref, send_sem.at[slot, n, 0], put_sem.at[slot, n, 0], next_x)

            def to_y(n):
                ref = part(n, core, column, slot)
                return remote(ref, ref, send_sem.at[slot, n, 1], put_sem.at[slot, n, 1], next_y)

            def on_y(n):
                ref = part(n, core, beside_x, slot, 0)
                return remote(ref, ref, send_sem.at[slot, n, 2], put_sem.at[slot, n, 2], next_y)

            def on_x(n):
                ref = part(n, core, beside_y, slot, 1)
                return remote(ref, ref, send_sem.at[slot, n, 3], put_sem.at[slot, n, 3], next_x)

            def to_peer(n, m):
                ref = part(n, core, [column, beside_x, beside_y, across][m], slot)
                return remote(ref, ref, send_sem.at[slot, n, 4 + m], peer_sem.at[slot, n, m], peer)

            def first(n):
                arrived(part(n, core, column, slot), get_sem.at[slot, n])
                to_x(n).start()
                to_y(n).start()
                to_peer(n, 0).start()

            def second(n):
                arrived(part(n, core, beside_x, slot), put_sem.at[slot, n, 0])
                on_y(n).start()
                to_peer(n, 1).start()
                arrived(part(n, core, beside_y, slot), put_sem.at[slot, n, 1])
                on_x(n).start()
                to_peer(n, 2).start()

            def third(n):
                arrived(part(n, core, across, slot, 0), put_sem.at[slot, n, 2])
                arrived(part(n, core, across, slot, 1), put_sem.at[slot, n, 3])
                to_peer(n, 3).start()

            def last(n):
                for m, c in enumerate([column, beside_x, beside_y, across]):
                    arrived(part(n, 1 - core, c, slot), peer_sem.at[slot, n, m])

            def sent(n):
                for copy in (to_x(n), to_y(n), on_y(n), on_x(n), *(to_peer(n, m) for m in range(4))):
                    copy.wait_send()

            return first, second, third, last, sent

        local = [pair // CORES == chip, (stages - 1 - pair) // CORES == chip]
        for slot in range(2):
            first, second, third, last, _ = gather(slot)

            @pl.when(local[slot])
            def _():
                for n in range(n_parts):
                    arrived(whole(n, slot), get_sem.at[slot, n])

            @pl.when(jnp.logical_not(local[slot]))
            def _():
                for n in range(n_parts + 2):
                    if n < n_parts:
                        first(n)
                    if 1 <= n <= n_parts:
                        second(n - 1)
                    if n >= 2:
                        third(n - 2)
                for n in range(n_parts):
                    last(n)

        t = Scratch()
        t.qkv, t.o, t.act, t.s, t.p = s_qkv, s_o, s_act, s_s, s_p
        channels = x_ref.shape[2]

        def a_copy(k):
            return remote(
                out_a.at[lax.rem(k, 2)], in_a.at[lax.rem(k + 1, SLOTS)], asend_sem.at[lax.rem(k, 2)],
                arecv_sem.at[lax.rem(k + 1, SLOTS)],
                {"data": group, "stage": lax.rem(chip + chips - 1, chips) * CORES + 1 - core},
            )

        def a_stay(k):
            slot = lax.rem(k + 1, SLOTS)
            return pltpu.make_async_copy(out_a.at[lax.rem(k, 2)], in_b.at[slot], brecv_sem.at[slot])

        def b_copy(k):
            return remote(
                out_b.at[lax.rem(k, 2)], in_b.at[lax.rem(k + 1, SLOTS)], bsend_sem.at[lax.rem(k, 2)],
                brecv_sem.at[lax.rem(k + 1, SLOTS)],
                {"data": group, "stage": lax.rem(chip + 1, chips) * CORES + 1 - core},
            )

        spread(all_mod[0, 0], mod_a)

        def step(k, _):
            slot = lax.rem(k, SLOTS)
            here, before = lax.rem(k, 2), lax.rem(k + 1, 2)

            @pl.when(k < steps - 1 - pair)
            def _():
                @pl.when(pair == 0)
                def _():
                    fill = jnp.zeros((CHUNK - channels, x_t.shape[1]), BF16)
                    h_ref[...] = product(w_in[...], jnp.concatenate([x_t[...].astype(BF16), fill], axis=0))

                @pl.when(pair > 0)
                def _():
                    @pl.when(k > 0)
                    def _():
                        arrived(in_a.at[slot], arecv_sem.at[slot])

                    h_ref[...] = in_a[slot].astype(F32)

                @pl.when(jnp.logical_and(k > 1, pair < last_pair))
                def _():
                    a_copy(k - 2).wait_send()

                block(h_ref, mod_a, all_w.at[0], out_a.at[here], t, heads, lambda: spread(all_mod[1, k], mod_b))

                @pl.when(pair == last_pair)
                def _():
                    a_stay(k).start()

                @pl.when(jnp.logical_and(pair < last_pair, k < steps - 3 - pair))
                def _():
                    a_copy(k).start()

            @pl.when(k == steps - 1 - pair)
            def _():
                spread(all_mod[1, k], mod_b)

            @pl.when(k > 0)
            def _():
                arrived(in_b.at[slot], brecv_sem.at[slot])

            @pl.when(jnp.logical_and(k > 1, pair > 0))
            def _():
                b_copy(k - 2).wait_send()

            h_ref[...] = product(w_skip[1], out_a[before]) + product(w_skip[0], in_b[slot])
            block(
                h_ref, mod_b, all_w.at[1], out_b.at[here], t, heads,
                lambda: spread(all_mod[0, jnp.minimum(k + 1, steps - 1)], mod_a),
            )

            @pl.when(pair > 0)
            def _():
                b_copy(k).start()

            @pl.when(pair == 0)
            def _():
                x_t[...] = keep_ref[k] * x_t[...] + noise_ref[k] * product(w_out[...], out_b[here])

            return 0

        lax.fori_loop(0, steps - pair, step, 0)

        def tell(n):
            return remote(x_t, x_all.at[sample], xsend_sem.at[n], xrecv_sem.at[sample], {"data": group, "stage": n})

        @pl.when(pair == 0)
        def _():
            for n in range(stages):

                @pl.when(n != me)
                def _():
                    tell(n).start()

            pltpu.make_async_copy(x_t, x_all.at[sample], xrecv_sem.at[sample]).start()

        count = steps - pair

        @pl.when(pair > 0)
        def _():
            b_copy(count - 2).wait_send()
            b_copy(count - 1).wait_send()

        for n in range(n_parts):

            @pl.when(goal == chip)
            def _():
                hand(n).wait_send()

            @pl.when(goal != chip)
            def _():
                for to_core in range(CORES):
                    leave(n, to_core).wait_send()

        for slot in range(2):

            @pl.when(jnp.logical_not(local[slot]))
            def _():
                for n in range(n_parts):
                    gather(slot)[4](n)

        @pl.when(pair == 0)
        def _():
            for n in range(stages):

                @pl.when(n != me)
                def _():
                    tell(n).wait_send()

        for n in range(CORES):
            arrived(x_all.at[n], xrecv_sem.at[n])
            out_ref[n] = x_all[n].T

    def local_run(x_init, h_warm, skip_warm, w_in, w_out, w_qkv, w_o, w_up, w_down, w_skip, ada_mods, keep, noise):
        batch, tokens, channels = x_init.shape
        width, ff = w_up.shape[1], w_up.shape[2]
        heads = w_o.shape[1]
        steps = ada_mods.shape[0]
        rows = 4 * width + 2 * ff
        any_ = pl.BlockSpec(memory_space=pl.ANY)
        vmem = pl.BlockSpec(memory_space=pltpu.VMEM)
        smem = pl.BlockSpec(memory_space=pltpu.SMEM)
        V = pltpu.VMEM
        D = pltpu.SemaphoreType.DMA
        scratch = [
            V((width, 3 * width), BF16), V((width, width), BF16), V((width, ff), BF16), V((ff, width), BF16),
            V((rows, width), BF16), V((steps, 6, width), F32), V((2, rows, width), BF16), V((2, steps, 6, width), F32),
            V((2 * width, width), BF16), V((2, width, width), BF16), V((3, tokens, width), BF16),
            V((width, CHUNK), BF16), V((channels, width), BF16),
            V((SLOTS, width, tokens), BF16), V((SLOTS, width, tokens), BF16),
            V((2, width, tokens), BF16), V((2, width, tokens), BF16),
            V((channels, tokens), F32), V((CORES, channels, tokens), F32), V((width, tokens), F32),
            V((3 * width, tokens), BF16), V((width, tokens), BF16), V((ff, tokens), BF16),
            V((2, tokens, tokens), F32), V((2, tokens, tokens), BF16),
            V((6, width, 128), F32), V((6, width, 128), F32),
            D((6,)), D((3,)), D((PIECES + 1, CORES)), D((2, PIECES + 1)), D((2, PIECES + 1, 8)), D((2, PIECES + 1, 4)),
            D((2, PIECES + 1, 4)),
            D((2,)), D((SLOTS,)), D((2,)), D((SLOTS,)), D((stages,)), D((CORES,)),
        ]
        call = pl.pallas_call(
            functools.partial(kernel, steps, heads),
            out_shape=jax.ShapeDtypeStruct((batch, tokens, channels), F32),
            in_specs=[vmem, any_, any_, vmem, vmem, any_, any_, any_, any_, any_, any_, smem, smem],
            out_specs=vmem,
            scratch_shapes=scratch,
            compiler_params=pltpu.CompilerParams(has_side_effects=True, vmem_limit_bytes=60 * 2**20),
            name="staged_sampler",
        )
        return call(
            x_init, h_warm, skip_warm, w_in, w_out, w_qkv, w_o.reshape(1, width, width), w_up, w_down, w_skip, ada_mods,
            keep, noise,
        )

    in_specs = (P('data'), P(None, 'data'), P(None, 'data'), P(), P(), P('stage'), P('stage'), P('stage'), P('stage'), P(), P(None, 'stage'), P(), P())
    return jax.shard_map(local_run, mesh=mesh, in_specs=in_specs, out_specs=P('data'), check_vma=False)
```

```python
import functools
import math

import jax
import jax.numpy as jnp
from jax import lax
from jax.experimental import pallas as pl
from jax.experimental.pallas import tpu as pltpu
from jax.sharding import PartitionSpec as P

F32 = jnp.float32
BF16 = jnp.bfloat16
CHUNK = 256
CORES = 2
COLUMNS = 4
PIECES = 6
LATE_OWN = (8, 9)
LATE_PEER = 3
SLOTS = 4
EPS = 1e-6
AHEAD = 3
TANH_A = math.sqrt(2.0 / math.pi)
TANH_B = TANH_A * 0.044715


def product(lhs, rhs):
    return jnp.dot(lhs, rhs, preferred_element_type=F32)


def norm_mod(h, scale, shift):
    width = h.shape[0]
    mean = jnp.sum(h, axis=0, keepdims=True) * (1.0 / width)
    c = h - mean
    var = jnp.sum(c * c, axis=0, keepdims=True) * (1.0 / width)
    return ((c * lax.rsqrt(var + EPS)) * scale + shift).astype(BF16)


def gelu(x):
    return (x * (0.5 + 0.5 * jnp.tanh(x * (TANH_A + TANH_B * (x * x))))).astype(BF16)


def softmax(s, scale):
    m = jnp.max(s, axis=0, keepdims=True)
    p = jnp.exp2((s - m) * (scale * math.log2(math.e)))
    return (p * (1.0 / jnp.sum(p, axis=0, keepdims=True))).astype(BF16)


def wide(cols):
    return jnp.concatenate([cols, cols], axis=1)


def spread(mods, half, dst):
    rows = dst.shape[1] // 128
    cols = mods.T
    cols = jnp.where(half == 0, cols[:, 0 : 3 * rows], cols[:, 3 * rows : 6 * rows])
    for v in range(3):
        for n in range(rows):
            col = cols[:, rows * v + n : rows * v + n + 1]
            if v == 1:
                col = 1.0 + col
            dst[3 * half + v, 128 * n : 128 * (n + 1), :] = jnp.broadcast_to(col, (128, 128))


def block(h_ref, mod, w, out, t, heads, extra):
    width, tokens = h_ref.shape
    dim = width // heads
    per_group = CHUNK // dim
    groups = heads // per_group
    row_o, row_up = 3 * width, 4 * width
    ff = (w.shape[0] - row_up) // 2
    row_down = row_up + ff

    u = norm_mod(h_ref[...], wide(mod[1]), wide(mod[0]))
    for row in (width, 0, 2 * width):
        t.qkv[row : row + width] = product(w[row : row + width], u).astype(BF16)

    zero = jnp.zeros((dim, tokens), BF16)
    keys = [t.qkv[width + CHUNK * g : width + CHUNK * (g + 1), :].T for g in range(groups)]
    order = [g * per_group + j for j in range(per_group) for g in range(groups)]

    def scores(n):
        g, j = divmod(order[n], per_group)
        query = t.qkv[dim * order[n] : dim * (order[n] + 1), :]
        padded = jnp.concatenate([query if m == j else zero for m in range(per_group)], axis=0)
        t.s[n % (AHEAD + 1)] = product(keys[g], padded)

    def probs(n):
        for c in range(0, tokens, 128):
            t.p[n % 2, :, c : c + 128] = softmax(t.s[n % (AHEAD + 1), :, c : c + 128], 1.0 / math.sqrt(dim))

    def values(n):
        row = dim * order[n]
        t.o[row : row + dim, :] = product(t.qkv[2 * width + row : 2 * width + row + dim, :], t.p[n % 2]).astype(BF16)

    for n in range(AHEAD):
        scores(n)
    for n in range(heads):
        if n + AHEAD < heads:
            scores(n + AHEAD)
        probs(n)
        values(n)

    for row in range(0, width, CHUNK):
        rows = slice(row, row + CHUNK)
        h_ref[rows] = h_ref[rows] + wide(mod[2, rows]) * product(w[row_o + row : row_o + row + CHUNK], t.o[...])
    u = norm_mod(h_ref[...], wide(mod[4]), wide(mod[3]))
    chunks = ff // CHUNK

    def up(n):
        return product(w[row_up + CHUNK * n : row_up + CHUNK * (n + 1)], u)

    held, total = up(0), None
    for n in range(chunks):
        ahead = up(n + 1) if n + 1 < chunks else None
        rows = slice(CHUNK * n, CHUNK * (n + 1))
        t.act[rows, :] = gelu(held)
        held = ahead
        if n == 0:
            extra()
        at, col = divmod(CHUNK * n, width)
        part = product(w[row_down + width * at : row_down + width * (at + 1), col : col + CHUNK], t.act[rows, :])
        total = part if total is None else total + part
    out[...] = (h_ref[...] + wide(mod[5]) * total).astype(BF16)


class Scratch:
    pass


def solution(mesh):
    stages = mesh.shape["stage"]
    chips = stages // CORES
    side = math.isqrt(mesh.shape["data"])
    if side * side != mesh.shape["data"] or side % 2:
        raise ValueError("data axis")

    def kernel(
        steps, heads,
        x_ref, hwarm_ref, swarm_ref, win_ref, wout_ref, wqkv_ref, wo_ref, wup_ref, wdown_ref, wskip_ref, mods_ref,
        keep_ref, noise_ref,
        out_ref,
        raw_qkv, raw_o, raw_up, raw_down, home_w, home_mod, all_w, all_mod,
        raw_skip, w_skip, raw_warm, w_in,
        hub, outs, x_t, x_end, h_ref, s_qkv, s_o, s_act, s_s, s_p, mod_b,
        load_sem, warm_sem, hsend_sem, get_sem, send_sem, put_sem,
        csend_sem, crecv_sem, ssend_sem, srecv_sem, xsend_sem, xrecv_sem, esend_sem, erecv_sem,
        late_sem, ccredit_sem, scredit_sem,
    ):
        me = lax.axis_index("stage")
        group = lax.axis_index("data")
        chip, core = me // CORES, lax.rem(me, CORES)
        pair = lax.rem(chips - chip, chips)
        first_half, second_half = core == 0, core == 1
        stage = jnp.where(first_half, pair, stages - 1 - pair)
        last_pair = chips - 1
        samples, channels = x_ref.shape[0], x_ref.shape[1]
        width = raw_o.shape[0]
        n_parts = PIECES + 1
        mod_rows = 6 * width // 128
        mesh_ids = pl.DeviceIdType.MESH

        odd_x, odd_y = lax.rem(group // side, 2), lax.rem(group, 2)
        column = 2 * odd_x + odd_y
        next_x = {"data": group + side * (1 - 2 * odd_x), "stage": me}
        next_y = {"data": group + 1 - 2 * odd_y, "stage": me}
        beside_x, beside_y = 2 * (1 - odd_x) + odd_y, 2 * odd_x + 1 - odd_y
        across = 2 * (1 - odd_x) + 1 - odd_y

        def device(chip_, core_):
            return {"data": group, "stage": chip_ * CORES + core_}

        peer = device(chip, 1 - core)
        chain_to = device(jnp.where(first_half, lax.rem(chip + chips - 1, chips), lax.rem(chip + 1, chips)), core)
        chain_from = device(jnp.where(first_half, lax.rem(chip + 1, chips), lax.rem(chip + chips - 1, chips)), core)

        def remote(src, dst, send, recv, to):
            return pltpu.make_async_remote_copy(
                src_ref=src, dst_ref=dst, send_sem=send, recv_sem=recv, device_id=to, device_id_type=mesh_ids
            )

        def arrived(ref, sem):
            pltpu.make_async_copy(ref, ref, sem).wait()

        raws = [raw_qkv, raw_o, raw_up, raw_down]
        homes = [wqkv_ref, wo_ref, wup_ref, wdown_ref]
        loads = [pltpu.make_async_copy(src.at[0], dst, load_sem.at[n]) for n, (src, dst) in enumerate(zip(homes, raws))]
        loads.append(pltpu.make_async_copy(mods_ref, home_mod, load_sem.at[4]))
        loads.append(pltpu.make_async_copy(wskip_ref.at[last_pair - pair], raw_skip, load_sem.at[5]))
        chain_warm = jnp.maximum(stage - 1, 0)
        warm = [
            pltpu.make_async_copy(hwarm_ref.at[chain_warm], raw_warm.at[0], warm_sem.at[0]),
            pltpu.make_async_copy(swarm_ref.at[pair], raw_warm.at[1], warm_sem.at[1]),
        ]
        for n in (4, 0, 1, 2, 3, 5):
            loads[n].start()
        for copy in warm:
            copy.start()

        def turn(src, dst, row):
            for at in range(0, src.shape[1], CHUNK):
                dst[row + at : row + at + CHUNK, :] = src[:, at : at + CHUNK].T

        home_pair = jnp.minimum(me, stages - 1 - me)
        goal_chip, goal_core = lax.rem(chips - home_pair, chips), jnp.where(me < chips, 0, 1)
        goal = device(goal_chip, goal_core)
        here = jnp.logical_and(goal_chip == chip, goal_core == core)
        beside = jnp.logical_and(goal_chip == chip, goal_core != core)
        away = goal_chip != chip
        is_local = stage // CORES == chip
        piece = home_w.shape[0] // PIECES

        def part(n, ref_w, ref_mod, column_=None, half=None):
            size, at = (ref_mod.shape[0], 0) if n == 0 else (piece, (n - 1) * piece)
            if column_ is not None:
                size //= COLUMNS
                at = at + column_ * size
            if half is not None:
                size //= 2
                at = at + half * size
            rows = pl.ds(at if isinstance(at, int) else pl.multiple_of(at, 8 if n == 0 else 16), size)
            return (ref_mod if n == 0 else ref_w).at[rows]

        def home(n, column_=None):
            return part(n, home_w, home_mod, column_)

        def mine(n, column_=None, half=None):
            return part(n, all_w, all_mod, column_, half)

        def stay(n):
            return pltpu.make_async_copy(home(n), mine(n), get_sem.at[n])

        def hand(n):
            return remote(home(n), mine(n), hsend_sem.at[n], get_sem.at[n], peer)

        def leave(n):
            return remote(home(n, column), mine(n, column), hsend_sem.at[n], get_sem.at[n], goal)

        late_own = functools.reduce(jnp.logical_or, [me == n for n in LATE_OWN])
        late_peer = me == LATE_PEER

        def send_now(n):
            @pl.when(here)
            def _():
                stay(n).start()

            @pl.when(beside)
            def _():
                hand(n).start()

            @pl.when(away)
            def _():
                leave(n).start()

        def send_home(n):
            @pl.when(jnp.logical_not(jnp.logical_or(late_own, late_peer)))
            def _():
                send_now(n)

        loads[4].wait()
        send_home(0)
        sent_to, row = 0, 0
        jobs = [(0, raw_qkv), (1, raw_o), (2, raw_up)]
        jobs += [(3, raw_down.at[width * n : width * (n + 1)]) for n in range(raw_down.shape[0] // width)]
        ready = -1
        for load, src in jobs:
            if load > ready:
                loads[load].wait()
                ready = load
            for col in range(0, src.shape[1], width):
                turn(src.at[:, col : col + width], home_w, row)
                row += width
                while (sent_to + 1) * piece <= row:
                    sent_to += 1
                    send_home(sent_to)

        def to_x(n):
            return remote(mine(n, column), mine(n, column), send_sem.at[n, 0], put_sem.at[n, 0], next_x)

        def to_y(n):
            return remote(mine(n, column), mine(n, column), send_sem.at[n, 1], put_sem.at[n, 1], next_y)

        def on_y(n):
            return remote(mine(n, beside_x, 0), mine(n, beside_x, 0), send_sem.at[n, 2], put_sem.at[n, 2], next_y)

        def on_x(n):
            return remote(mine(n, beside_y, 1), mine(n, beside_y, 1), send_sem.at[n, 3], put_sem.at[n, 3], next_x)

        @pl.when(late_peer)
        def _():
            pl.semaphore_wait(late_sem, 1)
            for n in range(n_parts):
                send_now(n)

        @pl.when(is_local)
        def _():
            for n in range(n_parts):
                arrived(mine(n), get_sem.at[n])

        @pl.when(jnp.logical_not(is_local))
        def _():
            for n in range(n_parts + 2):
                if n < n_parts:
                    arrived(mine(n, column), get_sem.at[n])
                    to_x(n).start()
                    to_y(n).start()
                if 1 <= n <= n_parts:
                    arrived(mine(n - 1, beside_x), put_sem.at[n - 1, 0])
                    on_y(n - 1).start()
                    arrived(mine(n - 1, beside_y), put_sem.at[n - 1, 1])
                    on_x(n - 1).start()
                if n >= 2:
                    arrived(mine(n - 2, across, 0), put_sem.at[n - 2, 2])
                    arrived(mine(n - 2, across, 1), put_sem.at[n - 2, 3])

        @pl.when(late_own)
        def _():
            for n in range(n_parts):
                send_now(n)

        @pl.when(me == LATE_PEER - 1)
        def _():
            pl.semaphore_signal(late_sem, inc=1, device_id=peer, device_id_type=mesh_ids)

        loads[5].wait()
        turn(raw_skip.at[0:width], w_skip.at[0], 0)
        turn(raw_skip.at[width : 2 * width], w_skip.at[1], 0)
        for copy in warm:
            copy.wait()
        for s in range(samples):
            hub[s, 0] = raw_warm[0, s].T
            hub[s, SLOTS] = raw_warm[1, s].T
            x_t[s, 0] = x_ref[s]
        w_in[...] = jnp.zeros_like(w_in)
        w_in[:, 0 : win_ref.shape[0]] = win_ref[...].T

        t = Scratch()
        t.qkv, t.o, t.act, t.s, t.p = s_qkv, s_o, s_act, s_s, s_p
        steps_a, steps_b = steps - 1 - pair, steps - pair
        count = jnp.where(first_half, steps_a, steps_b)
        chained = jnp.where(first_half, pair > 0, pair < last_pair)
        chains = jnp.where(first_half, pair < last_pair, pair > 0)
        chain_count = jnp.where(first_half, steps - 3 - pair, steps_b)

        def chain(k, s):
            slot = lax.rem(k + 1, SLOTS)
            return remote(outs.at[s, lax.rem(k, 2)], hub.at[s, slot], csend_sem.at[s, lax.rem(k, 2)], crecv_sem.at[s, slot], chain_to)

        def skip(k, s):
            slot = lax.rem(k + 1, SLOTS)
            return remote(outs.at[s, lax.rem(k, 2)], hub.at[s, SLOTS + slot], ssend_sem.at[s, lax.rem(k, 2)], srecv_sem.at[s, slot], peer)

        def latent(k, s):
            slot = lax.rem(k + 1, 2)
            return remote(x_t.at[s, slot], x_t.at[s, slot], xsend_sem.at[s, slot], xrecv_sem.at[s, slot], peer)

        def tell(n, s):
            return remote(x_end.at[s], x_end.at[s], esend_sem.at[s, n], erecv_sem.at[s], {"data": group, "stage": n})

        def mods_at(k):
            return all_mod[pl.ds(pl.multiple_of(k * mod_rows, 8), mod_rows)]

        for half in range(2):
            spread(mods_at(0), half, mod_b.at[0])

        def step(m, _):
            k, s = m // samples, lax.rem(m, samples)
            slot, at = lax.rem(k, SLOTS), lax.rem(k, 2)

            @pl.when(jnp.logical_and(k > 0, chained))
            def _():
                arrived(hub.at[s, slot], crecv_sem.at[s, slot])

            @pl.when(jnp.logical_and(first_half, pair == 0))
            def _():
                @pl.when(k > 0)
                def _():
                    arrived(x_t.at[s, at], xrecv_sem.at[s, at])

                fill = jnp.zeros((CHUNK - channels, x_t.shape[3]), BF16)
                x_pad = jnp.concatenate([x_t[s, at].astype(BF16), fill], axis=0)
                for row in range(0, width, CHUNK):
                    h_ref[row : row + CHUNK] = product(w_in[row : row + CHUNK], x_pad)

            @pl.when(jnp.logical_and(first_half, pair > 0))
            def _():
                h_ref[...] = hub[s, slot].astype(F32)

            @pl.when(second_half)
            def _():
                @pl.when(k > 0)
                def _():
                    arrived(hub.at[s, SLOTS + slot], srecv_sem.at[s, slot])

                main = jnp.where(jnp.logical_and(k > 0, pair == last_pair), SLOTS + slot, slot)
                for row in range(0, width, CHUNK):
                    rows = slice(row, row + CHUNK)
                    h_ref[rows] = product(w_skip[1, rows], hub[s, SLOTS + slot]) + product(w_skip[0, rows], hub[s, main])

                @pl.when(k + SLOTS < count)
                def _():
                    pl.semaphore_signal(scredit_sem.at[s], inc=1, device_id=peer, device_id_type=mesh_ids)

            @pl.when(jnp.logical_and(chained, k + SLOTS < count))
            def _():
                pl.semaphore_signal(ccredit_sem.at[s], inc=1, device_id=chain_from, device_id_type=mesh_ids)

            @pl.when(k > 1)
            def _():
                @pl.when(first_half)
                def _():
                    skip(k - 2, s).wait_send()

                @pl.when(chains)
                def _():
                    chain(k - 2, s).wait_send()

            block(
                h_ref, mod_b.at[at], all_w, outs.at[s, at], t, heads,
                lambda: spread(mods_at(jnp.minimum(k + 1, steps - 1)), s, mod_b.at[1 - at]),
            )

            @pl.when(jnp.logical_and(chains, k < chain_count))
            def _():
                @pl.when(k + 1 >= SLOTS)
                def _():
                    pl.semaphore_wait(ccredit_sem.at[s], 1)

                chain(k, s).start()

            @pl.when(first_half)
            def _():
                @pl.when(k + 1 >= SLOTS)
                def _():
                    pl.semaphore_wait(scredit_sem.at[s], 1)

                skip(k, s).start()

            @pl.when(jnp.logical_and(second_half, pair == 0))
            def _():
                @pl.when(k > 1)
                def _():
                    latent(k - 2, s).wait_send()

                noise = product(wout_ref[...], outs[s, at])
                x_new = keep_ref[k] * x_t[s, at] + noise_ref[k] * noise
                x_t[s, 1 - at] = x_new

                @pl.when(k < steps - 2)
                def _():
                    latent(k, s).start()

                @pl.when(k == steps - 1)
                def _():
                    x_end[s] = x_new
                    for n in range(stages):

                        @pl.when(n != me)
                        def _():
                            tell(n, s).start()

            return 0

        lax.fori_loop(0, count * samples, step, 0)

        for s in range(samples):
            for back in (2, 1):

                @pl.when(first_half)
                def _():
                    skip(count - back, s).wait_send()

                @pl.when(jnp.logical_and(second_half, chains))
                def _():
                    chain(count - back, s).wait_send()

        for n in range(n_parts):

            @pl.when(beside)
            def _():
                hand(n).wait_send()

            @pl.when(away)
            def _():
                leave(n).wait_send()

            @pl.when(jnp.logical_not(is_local))
            def _():
                for copy in (to_x(n), to_y(n), on_y(n), on_x(n)):
                    copy.wait_send()

        holder = jnp.logical_and(second_half, pair == 0)
        for s in range(samples):

            @pl.when(holder)
            def _():
                for n in range(stages):

                    @pl.when(n != me)
                    def _():
                        tell(n, s).wait_send()

            @pl.when(jnp.logical_not(holder))
            def _():
                arrived(x_end.at[s], erecv_sem.at[s])

            out_ref[s] = x_end[s]

    def local_run(x_init, h_warm, skip_warm, w_in, w_out, w_qkv, w_o, w_up, w_down, w_skip, ada_mods, keep, noise):
        batch, tokens, channels = x_init.shape
        width, ff = w_up.shape[1], w_up.shape[2]
        heads = w_o.shape[1]
        steps = ada_mods.shape[0]
        rows = 4 * width + 2 * ff
        mod_rows = 6 * width // 128
        any_ = pl.BlockSpec(memory_space=pl.ANY)
        vmem = pl.BlockSpec(memory_space=pltpu.VMEM)
        smem = pl.BlockSpec(memory_space=pltpu.SMEM)
        V = pltpu.VMEM
        D = pltpu.SemaphoreType.DMA
        R = pltpu.SemaphoreType.REGULAR
        parts = PIECES + 1
        scratch = [
            V((width, 3 * width), BF16), V((width, width), BF16), V((width, ff), BF16), V((ff, width), BF16),
            V((rows, width), BF16), V((steps * mod_rows, 128), F32), V((rows, width), BF16), V((steps * mod_rows, 128), F32),
            V((2 * width, width), BF16), V((2, width, width), BF16), V((2, batch, tokens, width), BF16), V((width, CHUNK), BF16),
            V((batch, 2 * SLOTS, width, tokens), BF16), V((batch, 2, width, tokens), BF16),
            V((batch, 2, channels, tokens), F32), V((batch, channels, tokens), F32), V((width, tokens), F32),
            V((3 * width, tokens), BF16), V((width, tokens), BF16), V((ff, tokens), BF16),
            V((AHEAD + 1, tokens, tokens), F32), V((2, tokens, tokens), BF16), V((2, 6, width, 128), F32),
            D((6,)), D((2,)), D((parts,)), D((parts,)), D((parts, 4)), D((parts, 4)),
            D((batch, 2)), D((batch, SLOTS)), D((batch, 2)), D((batch, SLOTS)), D((batch, 2)), D((batch, 2)),
            D((batch, stages)), D((batch,)), R, R((batch,)), R((batch,)),
        ]
        call = pl.pallas_call(
            functools.partial(kernel, steps, heads),
            out_shape=jax.ShapeDtypeStruct((batch, channels, tokens), F32),
            in_specs=[vmem, any_, any_, vmem, vmem, any_, any_, any_, any_, any_, any_, smem, smem],
            out_specs=vmem,
            scratch_shapes=scratch,
            compiler_params=pltpu.CompilerParams(has_side_effects=True, vmem_limit_bytes=60 * 2**20),
            name="staged_sampler",
        )
        made = call(
            x_init.swapaxes(1, 2), h_warm, skip_warm, w_in, w_out.T, w_qkv, w_o.reshape(1, width, width), w_up, w_down,
            w_skip, ada_mods.reshape(steps * mod_rows, 128), keep, noise,
        )
        return made.swapaxes(1, 2)

    in_specs = (P('data'), P(None, 'data'), P(None, 'data'), P(), P(), P('stage'), P('stage'), P('stage'), P('stage'), P(), P(None, 'stage'), P(), P())
    return jax.shard_map(local_run, mesh=mesh, in_specs=in_specs, out_specs=P('data'), check_vma=False)
```

```python
import functools
import math

import jax
import jax.numpy as jnp
from jax import lax
from jax.experimental import pallas as pl
from jax.experimental.pallas import tpu as pltpu
from jax.sharding import PartitionSpec as P

F32 = jnp.float32
BF16 = jnp.bfloat16
CHUNK = 256
CORES = 2
COLUMNS = 4
PIECES = 6
FIRST = 1
SLOTS = 4
EPS = 1e-6
AHEAD = 3
TANH_A = math.sqrt(2.0 / math.pi)
TANH_B = TANH_A * 0.044715


def product(lhs, rhs):
    return jnp.dot(lhs, rhs, preferred_element_type=F32)


def norm_mod(h, scale, shift):
    width = h.shape[0]
    mean = jnp.sum(h, axis=0, keepdims=True) * (1.0 / width)
    c = h - mean
    var = jnp.sum(c * c, axis=0, keepdims=True) * (1.0 / width)
    return ((c * lax.rsqrt(var + EPS)) * scale + shift).astype(BF16)


def gelu(x):
    return (x * (0.5 + 0.5 * jnp.tanh(x * (TANH_A + TANH_B * (x * x))))).astype(BF16)


def softmax(s, scale):
    m = jnp.max(s, axis=0, keepdims=True)
    p = jnp.exp2((s - m) * (scale * math.log2(math.e)))
    return (p * (1.0 / jnp.sum(p, axis=0, keepdims=True))).astype(BF16)


def wide(cols):
    return jnp.concatenate([cols, cols], axis=1)


def spread(mods, half, dst):
    rows = dst.shape[1] // 128
    cols = mods.T
    cols = jnp.where(half == 0, cols[:, 0 : 3 * rows], cols[:, 3 * rows : 6 * rows])
    for v in range(3):
        for n in range(rows):
            col = cols[:, rows * v + n : rows * v + n + 1]
            if v == 1:
                col = 1.0 + col
            dst[3 * half + v, 128 * n : 128 * (n + 1), :] = jnp.broadcast_to(col, (128, 128))


def block(h_ref, mod, w, out, t, heads, extra):
    width, tokens = h_ref.shape
    dim = width // heads
    per_group = CHUNK // dim
    groups = heads // per_group
    row_o, row_up = 3 * width, 4 * width
    ff = (w.shape[0] - row_up) // 2
    row_down = row_up + ff

    u = norm_mod(h_ref[...], wide(mod[1]), wide(mod[0]))
    for row in (width, 0, 2 * width):
        t.qkv[row : row + width] = product(w[row : row + width], u).astype(BF16)

    zero = jnp.zeros((dim, tokens), BF16)
    keys = [t.qkv[width + CHUNK * g : width + CHUNK * (g + 1), :].T for g in range(groups)]
    order = [g * per_group + j for j in range(per_group) for g in range(groups)]

    def scores(n):
        g, j = divmod(order[n], per_group)
        query = t.qkv[dim * order[n] : dim * (order[n] + 1), :]
        padded = jnp.concatenate([query if m == j else zero for m in range(per_group)], axis=0)
        t.s[n % (AHEAD + 1)] = product(keys[g], padded)

    def probs(n):
        for c in range(0, tokens, 128):
            t.p[n % 2, :, c : c + 128] = softmax(t.s[n % (AHEAD + 1), :, c : c + 128], 1.0 / math.sqrt(dim))

    def values(n):
        row = dim * order[n]
        t.o[row : row + dim, :] = product(t.qkv[2 * width + row : 2 * width + row + dim, :], t.p[n % 2]).astype(BF16)

    for n in range(AHEAD):
        scores(n)
    for n in range(heads):
        if n + AHEAD < heads:
            scores(n + AHEAD)
        probs(n)
        values(n)

    for row in range(0, width, CHUNK):
        rows = slice(row, row + CHUNK)
        h_ref[rows] = h_ref[rows] + wide(mod[2, rows]) * product(w[row_o + row : row_o + row + CHUNK], t.o[...])
    u = norm_mod(h_ref[...], wide(mod[4]), wide(mod[3]))
    chunks = ff // CHUNK

    def up(n):
        return product(w[row_up + CHUNK * n : row_up + CHUNK * (n + 1)], u)

    held, total = up(0), None
    for n in range(chunks):
        ahead = up(n + 1) if n + 1 < chunks else None
        rows = slice(CHUNK * n, CHUNK * (n + 1))
        t.act[rows, :] = gelu(held)
        held = ahead
        if n == 0:
            extra()
        at, col = divmod(CHUNK * n, width)
        part = product(w[row_down + width * at : row_down + width * (at + 1), col : col + CHUNK], t.act[rows, :])
        total = part if total is None else total + part
    out[...] = (h_ref[...] + wide(mod[5]) * total).astype(BF16)


class Scratch:
    pass


def solution(mesh):
    stages = mesh.shape["stage"]
    chips = stages // CORES
    side = math.isqrt(mesh.shape["data"])
    if side * side != mesh.shape["data"] or side % 2:
        raise ValueError("data axis")

    def kernel(
        steps, heads,
        x_ref, hwarm_ref, swarm_ref, win_ref, wout_ref, wqkv_ref, wo_ref, wup_ref, wdown_ref, wskip_ref, mods_ref,
        keep_ref, noise_ref,
        out_ref,
        raw_qkv, raw_o, raw_up, raw_down, home_w, home_mod, all_w, all_mod,
        raw_skip, w_skip, raw_warm, w_in,
        hub, outs, x_t, x_end, h_ref, s_qkv, s_o, s_act, s_s, s_p, mod_b,
        load_sem, warm_sem, hsend_sem, get_sem, send_sem, put_sem,
        csend_sem, crecv_sem, ssend_sem, srecv_sem, xsend_sem, xrecv_sem, esend_sem, erecv_sem,
        ccredit_sem, scredit_sem,
    ):
        me = lax.axis_index("stage")
        group = lax.axis_index("data")
        chip, core = me // CORES, lax.rem(me, CORES)
        pair = lax.rem(chips + FIRST - chip, chips)
        first_half, second_half = core == 0, core == 1
        stage = jnp.where(first_half, pair, stages - 1 - pair)
        last_pair = chips - 1
        samples, channels = x_ref.shape[0], x_ref.shape[1]
        width = raw_o.shape[0]
        n_parts = PIECES + 1
        mod_rows = 6 * width // 128
        mesh_ids = pl.DeviceIdType.MESH

        odd_x, odd_y = lax.rem(group // side, 2), lax.rem(group, 2)
        column = 2 * odd_x + odd_y
        next_x = {"data": group + side * (1 - 2 * odd_x), "stage": me}
        next_y = {"data": group + 1 - 2 * odd_y, "stage": me}
        beside_x, beside_y = 2 * (1 - odd_x) + odd_y, 2 * odd_x + 1 - odd_y
        across = 2 * (1 - odd_x) + 1 - odd_y

        def device(chip_, core_):
            return {"data": group, "stage": chip_ * CORES + core_}

        peer = device(chip, 1 - core)
        chain_to = device(jnp.where(first_half, lax.rem(chip + chips - 1, chips), lax.rem(chip + 1, chips)), core)
        chain_from = device(jnp.where(first_half, lax.rem(chip + 1, chips), lax.rem(chip + chips - 1, chips)), core)

        def remote(src, dst, send, recv, to):
            return pltpu.make_async_remote_copy(
                src_ref=src, dst_ref=dst, send_sem=send, recv_sem=recv, device_id=to, device_id_type=mesh_ids
            )

        def arrived(ref, sem):
            pltpu.make_async_copy(ref, ref, sem).wait()

        barrier = pltpu.get_barrier_semaphore()
        for n in range(1, stages):
            pl.semaphore_signal(
                barrier, inc=1, device_id={"data": group, "stage": lax.rem(me + n, stages)}, device_id_type=mesh_ids
            )
        for beyond in (next_x, next_y):
            pl.semaphore_signal(barrier, inc=1, device_id=beyond, device_id_type=mesh_ids)

        raws = [raw_qkv, raw_o, raw_up, raw_down]
        homes = [wqkv_ref, wo_ref, wup_ref, wdown_ref]
        loads = [pltpu.make_async_copy(src.at[0], dst, load_sem.at[n]) for n, (src, dst) in enumerate(zip(homes, raws))]
        loads.append(pltpu.make_async_copy(mods_ref, home_mod, load_sem.at[4]))
        loads.append(pltpu.make_async_copy(wskip_ref.at[last_pair - pair], raw_skip, load_sem.at[5]))
        chain_warm = jnp.maximum(stage - 1, 0)
        warm = [
            pltpu.make_async_copy(hwarm_ref.at[chain_warm], raw_warm.at[0], warm_sem.at[0]),
            pltpu.make_async_copy(swarm_ref.at[pair], raw_warm.at[1], warm_sem.at[1]),
        ]
        for n in (4, 0, 1, 2, 3, 5):
            loads[n].start()
        for copy in warm:
            copy.start()

        def turn(src, dst, row):
            for at in range(0, src.shape[1], CHUNK):
                dst[row + at : row + at + CHUNK, :] = src[:, at : at + CHUNK].T

        home_pair = jnp.minimum(me, stages - 1 - me)
        goal_chip, goal_core = lax.rem(chips + FIRST - home_pair, chips), jnp.where(me < chips, 0, 1)
        goal = device(goal_chip, goal_core)
        here = jnp.logical_and(goal_chip == chip, goal_core == core)
        beside = jnp.logical_and(goal_chip == chip, goal_core != core)
        away = goal_chip != chip
        is_local = stage // CORES == chip
        piece = home_w.shape[0] // PIECES

        def part(n, ref_w, ref_mod, column_=None, third=None):
            size, at = (ref_mod.shape[0], 0) if n == 0 else (piece, (n - 1) * piece)
            if column_ is not None:
                size //= COLUMNS
                at = at + column_ * size
            if third is not None:
                unit = 8 if n == 0 else 16
                least = size // (3 * unit) * unit
                size, shift = [(size - 2 * least, 0), (least, size - 2 * least), (least, size - least)][third]
                at = at + shift
            rows = pl.ds(at if isinstance(at, int) else pl.multiple_of(at, 8 if n == 0 else 16), size)
            return (ref_mod if n == 0 else ref_w).at[rows]

        def home(n, column_=None, third=None):
            return part(n, home_w, home_mod, column_, third)

        def mine(n, column_=None, third=None):
            return part(n, all_w, all_mod, column_, third)

        def stay(n):
            return pltpu.make_async_copy(home(n), mine(n), get_sem.at[n, 0])

        def hand(n):
            return remote(home(n), mine(n), hsend_sem.at[n, 0], get_sem.at[n, 0], peer)

        def leave(n):
            return remote(home(n, column), mine(n, column), hsend_sem.at[n, 0], get_sem.at[n, 0], goal)

        def leave_more(n):
            return remote(home(n, across, 0), mine(n, across, 0), hsend_sem.at[n, 1], get_sem.at[n, 1], goal)

        def send_now(n):
            @pl.when(here)
            def _():
                stay(n).start()

            @pl.when(beside)
            def _():
                hand(n).start()

            @pl.when(away)
            def _():
                leave(n).start()
                leave_more(n).start()

        loads[4].wait()
        sent, row = -1, 0
        jobs = [(0, raw_qkv), (1, raw_o), (2, raw_up)]
        jobs += [(3, raw_down.at[width * n : width * (n + 1)]) for n in range(raw_down.shape[0] // width)]
        ready = -1
        for load, src in jobs:
            if load > ready:
                loads[load].wait()
                ready = load
            for col in range(0, src.shape[1], width):
                turn(src.at[:, col : col + width], home_w, row)
                row += width
                while (sent + 1) * piece <= row:
                    if sent < 0:
                        pl.semaphore_wait(barrier, stages + 1)
                    sent += 1
                    send_now(sent)

        def to_x(n):
            return remote(mine(n, column), mine(n, column), send_sem.at[n, 0], put_sem.at[n, 0], next_x)

        def to_y(n):
            return remote(mine(n, column), mine(n, column), send_sem.at[n, 1], put_sem.at[n, 1], next_y)

        def on_y(n):
            return remote(mine(n, beside_x, 1), mine(n, beside_x, 1), send_sem.at[n, 2], put_sem.at[n, 2], next_y)

        def on_x(n):
            return remote(mine(n, beside_y, 2), mine(n, beside_y, 2), send_sem.at[n, 3], put_sem.at[n, 3], next_x)

        @pl.when(is_local)
        def _():
            for n in range(n_parts):
                arrived(mine(n), get_sem.at[n, 0])

        @pl.when(jnp.logical_not(is_local))
        def _():
            for n in range(n_parts + 2):
                if n < n_parts:
                    arrived(mine(n, column), get_sem.at[n, 0])
                    to_x(n).start()
                    to_y(n).start()
                if 1 <= n <= n_parts:
                    arrived(mine(n - 1, beside_x), put_sem.at[n - 1, 0])
                    on_y(n - 1).start()
                    arrived(mine(n - 1, beside_y), put_sem.at[n - 1, 1])
                    on_x(n - 1).start()
                if n >= 2:
                    arrived(mine(n - 2, across, 0), get_sem.at[n - 2, 1])
                    arrived(mine(n - 2, across, 1), put_sem.at[n - 2, 2])
                    arrived(mine(n - 2, across, 2), put_sem.at[n - 2, 3])

        loads[5].wait()
        turn(raw_skip.at[0:width], w_skip.at[0], 0)
        turn(raw_skip.at[width : 2 * width], w_skip.at[1], 0)
        for copy in warm:
            copy.wait()
        for s in range(samples):
            hub[s, 0] = raw_warm[0, s].T
            hub[s, SLOTS] = raw_warm[1, s].T
            x_t[s, 0] = x_ref[s]
        w_in[...] = jnp.zeros_like(w_in)
        w_in[:, 0 : win_ref.shape[0]] = win_ref[...].T

        t = Scratch()
        t.qkv, t.o, t.act, t.s, t.p = s_qkv, s_o, s_act, s_s, s_p
        steps_a, steps_b = steps - 1 - pair, steps - pair
        count = jnp.where(first_half, steps_a, steps_b)
        chained = jnp.where(first_half, pair > 0, pair < last_pair)
        chains = jnp.where(first_half, pair < last_pair, pair > 0)
        chain_count = jnp.where(first_half, steps - 3 - pair, steps_b)

        def chain(k, s):
            slot = lax.rem(k + 1, SLOTS)
            return remote(outs.at[s, lax.rem(k, 2)], hub.at[s, slot], csend_sem.at[s, lax.rem(k, 2)], crecv_sem.at[s, slot], chain_to)

        def skip(k, s):
            slot = lax.rem(k + 1, SLOTS)
            return remote(outs.at[s, lax.rem(k, 2)], hub.at[s, SLOTS + slot], ssend_sem.at[s, lax.rem(k, 2)], srecv_sem.at[s, slot], peer)

        def latent(k, s):
            slot = lax.rem(k + 1, 2)
            return remote(x_t.at[s, slot], x_t.at[s, slot], xsend_sem.at[s, slot], xrecv_sem.at[s, slot], peer)

        def tell(n, s):
            return remote(x_end.at[s], x_end.at[s], esend_sem.at[s, n], erecv_sem.at[s], {"data": group, "stage": n})

        def mods_at(k):
            return all_mod[pl.ds(pl.multiple_of(k * mod_rows, 8), mod_rows)]

        for half in range(2):
            spread(mods_at(0), half, mod_b.at[0])

        def step(m, _):
            k, s = m // samples, lax.rem(m, samples)
            slot, at = lax.rem(k, SLOTS), lax.rem(k, 2)

            @pl.when(jnp.logical_and(k > 0, chained))
            def _():
                arrived(hub.at[s, slot], crecv_sem.at[s, slot])

            @pl.when(jnp.logical_and(first_half, pair == 0))
            def _():
                @pl.when(k > 0)
                def _():
                    arrived(x_t.at[s, at], xrecv_sem.at[s, at])

                fill = jnp.zeros((CHUNK - channels, x_t.shape[3]), BF16)
                x_pad = jnp.concatenate([x_t[s, at].astype(BF16), fill], axis=0)
                for row in range(0, width, CHUNK):
                    h_ref[row : row + CHUNK] = product(w_in[row : row + CHUNK], x_pad)

            @pl.when(jnp.logical_and(first_half, pair > 0))
            def _():
                h_ref[...] = hub[s, slot].astype(F32)

            @pl.when(second_half)
            def _():
                @pl.when(k > 0)
                def _():
                    arrived(hub.at[s, SLOTS + slot], srecv_sem.at[s, slot])

                main = jnp.where(jnp.logical_and(k > 0, pair == last_pair), SLOTS + slot, slot)
                for row in range(0, width, CHUNK):
                    rows = slice(row, row + CHUNK)
                    h_ref[rows] = product(w_skip[1, rows], hub[s, SLOTS + slot]) + product(w_skip[0, rows], hub[s, main])

                @pl.when(k + SLOTS < count)
                def _():
                    pl.semaphore_signal(scredit_sem.at[s], inc=1, device_id=peer, device_id_type=mesh_ids)

            @pl.when(jnp.logical_and(chained, k + SLOTS < count))
            def _():
                pl.semaphore_signal(ccredit_sem.at[s], inc=1, device_id=chain_from, device_id_type=mesh_ids)

            @pl.when(k > 1)
            def _():
                @pl.when(first_half)
                def _():
                    skip(k - 2, s).wait_send()

                @pl.when(chains)
                def _():
                    chain(k - 2, s).wait_send()

            block(
                h_ref, mod_b.at[at], all_w, outs.at[s, at], t, heads,
                lambda: spread(mods_at(jnp.minimum(k + 1, steps - 1)), s, mod_b.at[1 - at]),
            )

            @pl.when(jnp.logical_and(chains, k < chain_count))
            def _():
                @pl.when(k + 1 >= SLOTS)
                def _():
                    pl.semaphore_wait(ccredit_sem.at[s], 1)

                chain(k, s).start()

            @pl.when(first_half)
            def _():
                @pl.when(k + 1 >= SLOTS)
                def _():
                    pl.semaphore_wait(scredit_sem.at[s], 1)

                skip(k, s).start()

            @pl.when(jnp.logical_and(second_half, pair == 0))
            def _():
                @pl.when(k > 1)
                def _():
                    latent(k - 2, s).wait_send()

                noise = product(wout_ref[...], outs[s, at])
                x_new = keep_ref[k] * x_t[s, at] + noise_ref[k] * noise
                x_t[s, 1 - at] = x_new

                @pl.when(k < steps - 2)
                def _():
                    latent(k, s).start()

                @pl.when(k == steps - 1)
                def _():
                    x_end[s] = x_new
                    for n in range(stages):

                        @pl.when(n != me)
                        def _():
                            tell(n, s).start()

            return 0

        lax.fori_loop(0, count * samples, step, 0)

        for s in range(samples):
            for back in (2, 1):

                @pl.when(first_half)
                def _():
                    skip(count - back, s).wait_send()

                @pl.when(jnp.logical_and(second_half, chains))
                def _():
                    chain(count - back, s).wait_send()

        for n in range(n_parts):

            @pl.when(beside)
            def _():
                hand(n).wait_send()

            @pl.when(away)
            def _():
                leave(n).wait_send()
                leave_more(n).wait_send()

            @pl.when(jnp.logical_not(is_local))
            def _():
                for copy in (to_x(n), to_y(n), on_y(n), on_x(n)):
                    copy.wait_send()

        holder = jnp.logical_and(second_half, pair == 0)
        for s in range(samples):

            @pl.when(holder)
            def _():
                for n in range(stages):

                    @pl.when(n != me)
                    def _():
                        tell(n, s).wait_send()

            @pl.when(jnp.logical_not(holder))
            def _():
                arrived(x_end.at[s], erecv_sem.at[s])

            out_ref[s] = x_end[s]

    def local_run(x_init, h_warm, skip_warm, w_in, w_out, w_qkv, w_o, w_up, w_down, w_skip, ada_mods, keep, noise):
        batch, tokens, channels = x_init.shape
        width, ff = w_up.shape[1], w_up.shape[2]
        heads = w_o.shape[1]
        steps = ada_mods.shape[0]
        rows = 4 * width + 2 * ff
        mod_rows = 6 * width // 128
        any_ = pl.BlockSpec(memory_space=pl.ANY)
        vmem = pl.BlockSpec(memory_space=pltpu.VMEM)
        smem = pl.BlockSpec(memory_space=pltpu.SMEM)
        V = pltpu.VMEM
        D = pltpu.SemaphoreType.DMA
        R = pltpu.SemaphoreType.REGULAR
        parts = PIECES + 1
        scratch = [
            V((width, 3 * width), BF16), V((width, width), BF16), V((width, ff), BF16), V((ff, width), BF16),
            V((rows, width), BF16), V((steps * mod_rows, 128), F32), V((rows, width), BF16), V((steps * mod_rows, 128), F32),
            V((2 * width, width), BF16), V((2, width, width), BF16), V((2, batch, tokens, width), BF16), V((width, CHUNK), BF16),
            V((batch, 2 * SLOTS, width, tokens), BF16), V((batch, 2, width, tokens), BF16),
            V((batch, 2, channels, tokens), F32), V((batch, channels, tokens), F32), V((width, tokens), F32),
            V((3 * width, tokens), BF16), V((width, tokens), BF16), V((ff, tokens), BF16),
            V((AHEAD + 1, tokens, tokens), F32), V((2, tokens, tokens), BF16), V((2, 6, width, 128), F32),
            D((6,)), D((2,)), D((parts, 2)), D((parts, 2)), D((parts, 4)), D((parts, 4)),
            D((batch, 2)), D((batch, SLOTS)), D((batch, 2)), D((batch, SLOTS)), D((batch, 2)), D((batch, 2)),
            D((batch, stages)), D((batch,)), R((batch,)), R((batch,)),
        ]
        call = pl.pallas_call(
            functools.partial(kernel, steps, heads),
            out_shape=jax.ShapeDtypeStruct((batch, channels, tokens), F32),
            in_specs=[vmem, any_, any_, vmem, vmem, any_, any_, any_, any_, any_, any_, smem, smem],
            out_specs=vmem,
            scratch_shapes=scratch,
            compiler_params=pltpu.CompilerParams(collective_id=0, has_side_effects=True, vmem_limit_bytes=60 * 2**20),
            name="staged_sampler",
        )
        made = call(
            x_init.swapaxes(1, 2), h_warm, skip_warm, w_in, w_out.T, w_qkv, w_o.reshape(1, width, width), w_up, w_down,
            w_skip, ada_mods.reshape(steps * mod_rows, 128), keep, noise,
        )
        return made.swapaxes(1, 2)

    in_specs = (P('data'), P(None, 'data'), P(None, 'data'), P(), P(), P('stage'), P('stage'), P('stage'), P('stage'), P(), P(None, 'stage'), P(), P())
    return jax.shard_map(local_run, mesh=mesh, in_specs=in_specs, out_specs=P('data'), check_vma=False)
```

```python
import functools
import math

import jax
import jax.numpy as jnp
from jax import lax
from jax.experimental import pallas as pl
from jax.experimental.pallas import tpu as pltpu
from jax.sharding import PartitionSpec as P

F32 = jnp.float32
BF16 = jnp.bfloat16
CHUNK = 256
CORES = 2
COLUMNS = 4
PIECES = (4, 8, 8, 8, 8, 7, 5)
FIRST = 1
SLOTS = 4
EPS = 1e-6
AHEAD = 5
UP_AHEAD = 2
DOWN_BEHIND = 1
TANH_A = math.sqrt(2.0 / math.pi)
TANH_B = TANH_A * 0.044715


def product(lhs, rhs):
    return jnp.dot(lhs, rhs, preferred_element_type=F32)


def norm_mod(h_ref, scale, shift):
    width = h_ref.shape[0]

    def total(term):
        sums = [None] * 4
        for n, row in enumerate(range(0, width, 8)):
            v = term(h_ref[row : row + 8, :])
            sums[n % 4] = v if sums[n % 4] is None else sums[n % 4] + v
        return jnp.sum((sums[0] + sums[1]) + (sums[2] + sums[3]), axis=0, keepdims=True) * (1.0 / width)

    mean = total(lambda v: v)
    rate = lax.rsqrt(total(lambda v: (v - mean) * (v - mean)) + EPS)
    rows = [slice(row, row + 16) for row in range(0, width, 16)]
    return jnp.concatenate(
        [(((h_ref[r, :] - mean) * rate) * wide(scale[r]) + wide(shift[r])).astype(BF16) for r in rows], axis=0
    )


def gelu(x):
    return (x * (0.5 + 0.5 * jnp.tanh(x * (TANH_A + TANH_B * (x * x))))).astype(BF16)


def softmax(s, scale):
    m = jnp.max(s, axis=0, keepdims=True)
    p = jnp.exp2((s - m) * (scale * math.log2(math.e)))
    return p.astype(BF16), 1.0 / jnp.sum(p, axis=0, keepdims=True)


def wide(cols):
    return jnp.concatenate([cols, cols], axis=1)


def spread(mods, half, dst):
    rows = dst.shape[1] // 128
    cols = mods.T
    cols = jnp.where(half == 0, cols[:, 0 : 3 * rows], cols[:, 3 * rows : 6 * rows])
    for v in range(3):
        for n in range(rows):
            col = cols[:, rows * v + n : rows * v + n + 1]
            if v == 1:
                col = 1.0 + col
            dst[3 * half + v, 128 * n : 128 * (n + 1), :] = jnp.broadcast_to(col, (128, 128))


def block(h_ref, mod, w, out, t, heads, extra):
    width, tokens = h_ref.shape
    dim = width // heads
    per_group = CHUNK // dim
    groups = heads // per_group
    row_o, row_up = 3 * width, 4 * width
    ff = (w.shape[0] - row_up) // 2
    row_down = row_up + ff

    u = norm_mod(h_ref, mod[1], mod[0])
    for row, size in [(width + CHUNK * g, CHUNK) if n == 0 else (CHUNK * g, CHUNK) for g in range(groups) for n in range(2)] + [
        (2 * width, width)
    ]:
        t.qkv[row : row + size] = product(w[row : row + size], u).astype(BF16)

    zero = jnp.zeros((dim, tokens), BF16)
    keys, rate = {}, {}

    def scores(hd):
        g, j = divmod(hd, per_group)
        if g not in keys:
            keys[g] = t.qkv[width + CHUNK * g : width + CHUNK * (g + 1), :].T
        query = t.qkv[dim * hd : dim * (hd + 1), :]
        padded = jnp.concatenate([query if m == j else zero for m in range(per_group)], axis=0)
        t.s[hd % (AHEAD + 1)] = product(keys[g], padded)

    def probs(hd):
        t.p[hd % 2], rate[hd] = softmax(t.s[hd % (AHEAD + 1)], 1.0 / math.sqrt(dim))

    def values(hd):
        row = dim * hd
        v = product(t.qkv[2 * width + row : 2 * width + row + dim, :], t.p[hd % 2])
        t.o[row : row + dim, :] = (v * rate[hd]).astype(BF16)

    for n in range(AHEAD):
        scores(n)
    for n in range(heads):
        if n + AHEAD < heads:
            scores(n + AHEAD)
        probs(n)
        values(n)

    for row in range(0, width, CHUNK):
        rows = slice(row, row + CHUNK)
        h_ref[rows] = h_ref[rows] + wide(mod[2, rows]) * product(w[row_o + row : row_o + row + CHUNK], t.o[...])
    u = norm_mod(h_ref, mod[4], mod[3])
    chunks = ff // CHUNK
    held, total = {}, [None] * (width // CHUNK)

    def up(n):
        held[n] = product(w[row_up + CHUNK * n : row_up + CHUNK * (n + 1)], u)

    def down(n):
        at, col = divmod(CHUNK * n, width)
        for q in range(len(total)):
            row = row_down + width * at + CHUNK * q
            part = product(w[row : row + CHUNK, col : col + CHUNK], t.act[CHUNK * n : CHUNK * (n + 1), :])
            total[q] = part if total[q] is None else total[q] + part

    for n in range(UP_AHEAD):
        up(n)
    for n in range(chunks):
        if n + UP_AHEAD < chunks:
            up(n + UP_AHEAD)
        t.act[CHUNK * n : CHUNK * (n + 1), :] = gelu(held.pop(n))
        if n == 0:
            extra()
        if n >= DOWN_BEHIND:
            down(n - DOWN_BEHIND)
    for n in range(chunks - DOWN_BEHIND, chunks):
        down(n)
    for q, v in enumerate(total):
        rows = slice(CHUNK * q, CHUNK * (q + 1))
        out[rows] = (h_ref[rows] + wide(mod[5, rows]) * v).astype(BF16)


class Scratch:
    pass


def solution(mesh):
    stages = mesh.shape["stage"]
    chips = stages // CORES
    side = math.isqrt(mesh.shape["data"])
    if side * side != mesh.shape["data"] or side % 2:
        raise ValueError("data axis")

    def kernel(
        steps, heads,
        x_ref, hwarm_ref, swarm_ref, win_ref, wout_ref, wqkv_ref, wo_ref, wup_ref, wdown_ref, wskip_ref, mods_ref,
        keep_ref, noise_ref,
        out_ref,
        raw_qkv, raw_o, raw_up, raw_down, home_w, home_mod, all_w, all_mod,
        raw_skip, w_skip, raw_warm, w_in,
        hub, outs, x_t, x_end, h_ref, s_qkv, s_o, s_act, s_s, s_p, mod_b,
        load_sem, warm_sem, hsend_sem, get_sem, send_sem, put_sem,
        csend_sem, crecv_sem, ssend_sem, srecv_sem, xsend_sem, xrecv_sem, esend_sem, erecv_sem,
        ccredit_sem, scredit_sem,
    ):
        me = lax.axis_index("stage")
        group = lax.axis_index("data")
        chip, core = me // CORES, lax.rem(me, CORES)
        pair = lax.rem(chips + FIRST - chip, chips)
        first_half, second_half = core == 0, core == 1
        stage = jnp.where(first_half, pair, stages - 1 - pair)
        last_pair = chips - 1
        samples, channels = x_ref.shape[0], x_ref.shape[1]
        width = raw_o.shape[0]
        n_parts = len(PIECES) + 1
        mod_rows = 6 * width // 128
        mesh_ids = pl.DeviceIdType.MESH

        odd_x, odd_y = lax.rem(group // side, 2), lax.rem(group, 2)
        column = 2 * odd_x + odd_y
        next_x = {"data": group + side * (1 - 2 * odd_x), "stage": me}
        next_y = {"data": group + 1 - 2 * odd_y, "stage": me}
        beside_x, beside_y = 2 * (1 - odd_x) + odd_y, 2 * odd_x + 1 - odd_y
        across = 2 * (1 - odd_x) + 1 - odd_y

        def device(chip_, core_):
            return {"data": group, "stage": chip_ * CORES + core_}

        peer = device(chip, 1 - core)
        chain_to = device(jnp.where(first_half, lax.rem(chip + chips - 1, chips), lax.rem(chip + 1, chips)), core)
        chain_from = device(jnp.where(first_half, lax.rem(chip + 1, chips), lax.rem(chip + chips - 1, chips)), core)

        def remote(src, dst, send, recv, to):
            return pltpu.make_async_remote_copy(
                src_ref=src, dst_ref=dst, send_sem=send, recv_sem=recv, device_id=to, device_id_type=mesh_ids
            )

        def arrived(ref, sem):
            pltpu.make_async_copy(ref, ref, sem).wait()

        barrier = pltpu.get_barrier_semaphore()
        for n in range(1, stages):
            pl.semaphore_signal(
                barrier, inc=1, device_id={"data": group, "stage": lax.rem(me + n, stages)}, device_id_type=mesh_ids
            )
        for beyond in (next_x, next_y):
            pl.semaphore_signal(barrier, inc=1, device_id=beyond, device_id_type=mesh_ids)

        raws = [raw_qkv, raw_o, raw_up, raw_down]
        homes = [wqkv_ref, wo_ref, wup_ref, wdown_ref]
        loads = [pltpu.make_async_copy(src.at[0], dst, load_sem.at[n]) for n, (src, dst) in enumerate(zip(homes, raws))]
        loads.append(pltpu.make_async_copy(mods_ref, home_mod, load_sem.at[4]))
        loads.append(pltpu.make_async_copy(wskip_ref.at[last_pair - pair], raw_skip, load_sem.at[5]))
        chain_warm = jnp.maximum(stage - 1, 0)
        warm = [
            pltpu.make_async_copy(hwarm_ref.at[chain_warm], raw_warm.at[0], warm_sem.at[0]),
            pltpu.make_async_copy(swarm_ref.at[pair], raw_warm.at[1], warm_sem.at[1]),
        ]
        for n in (4, 0, 1, 2, 3, 5):
            loads[n].start()
        for copy in warm:
            copy.start()

        def turn(src, dst, row):
            for at in range(0, src.shape[1], CHUNK):
                dst[row + at : row + at + CHUNK, :] = src[:, at : at + CHUNK].T

        home_pair = jnp.minimum(me, stages - 1 - me)
        goal_chip, goal_core = lax.rem(chips + FIRST - home_pair, chips), jnp.where(me < chips, 0, 1)
        goal = device(goal_chip, goal_core)
        here = jnp.logical_and(goal_chip == chip, goal_core == core)
        beside = jnp.logical_and(goal_chip == chip, goal_core != core)
        away = goal_chip != chip
        is_local = stage // CORES == chip
        shared = n_parts - 1
        ends = [home_w.shape[0] * sum(PIECES[:n]) // sum(PIECES) for n in range(n_parts)]

        def part(n, ref_w, ref_mod, column_=None, half=None):
            size, at = (ref_mod.shape[0], 0) if n == 0 else (ends[n] - ends[n - 1], ends[n - 1])
            if column_ is not None:
                size //= COLUMNS
                at = at + column_ * size
            if half is not None:
                size //= 2
                at = at + half * size
            rows = pl.ds(at if isinstance(at, int) else pl.multiple_of(at, 8 if n == 0 else 16), size)
            return (ref_mod if n == 0 else ref_w).at[rows]

        def home(n, column_=None):
            return part(n, home_w, home_mod, column_)

        def mine(n, column_=None, half=None):
            return part(n, all_w, all_mod, column_, half)

        def stay(n):
            return pltpu.make_async_copy(home(n), mine(n), get_sem.at[n])

        def hand(n):
            return remote(home(n), mine(n), hsend_sem.at[n], get_sem.at[n], peer)

        def leave(n):
            which = column if n < shared else None
            return remote(home(n, which), mine(n, which), hsend_sem.at[n], get_sem.at[n], goal)

        def send_now(n):
            @pl.when(here)
            def _():
                stay(n).start()

            @pl.when(beside)
            def _():
                hand(n).start()

            @pl.when(away)
            def _():
                leave(n).start()

        loads[4].wait()
        sent, row = -1, 0
        jobs = [(0, raw_qkv), (1, raw_o), (2, raw_up)]
        jobs += [(3, raw_down.at[width * n : width * (n + 1)]) for n in range(raw_down.shape[0] // width)]
        ready = -1
        for load, src in jobs:
            if load > ready:
                loads[load].wait()
                ready = load
            for col in range(0, src.shape[1], width):
                turn(src.at[:, col : col + width], home_w, row)
                row += width
                while sent + 1 < n_parts and ends[sent + 1] <= row:
                    if sent < 0:
                        pl.semaphore_wait(barrier, stages + 1)
                    sent += 1
                    send_now(sent)

        def to_x(n):
            return remote(mine(n, column), mine(n, column), send_sem.at[n, 0], put_sem.at[n, 0], next_x)

        def to_y(n):
            return remote(mine(n, column), mine(n, column), send_sem.at[n, 1], put_sem.at[n, 1], next_y)

        def on_y(n):
            return remote(mine(n, beside_x, 0), mine(n, beside_x, 0), send_sem.at[n, 2], put_sem.at[n, 2], next_y)

        def on_x(n):
            return remote(mine(n, beside_y, 1), mine(n, beside_y, 1), send_sem.at[n, 3], put_sem.at[n, 3], next_x)

        @pl.when(is_local)
        def _():
            for n in range(n_parts):
                arrived(mine(n), get_sem.at[n])

        @pl.when(jnp.logical_not(is_local))
        def _():
            for n in range(shared + 2):
                if n < shared:
                    arrived(mine(n, column), get_sem.at[n])
                    to_x(n).start()
                    to_y(n).start()
                if 1 <= n <= shared:
                    arrived(mine(n - 1, beside_x), put_sem.at[n - 1, 0])
                    on_y(n - 1).start()
                    arrived(mine(n - 1, beside_y), put_sem.at[n - 1, 1])
                    on_x(n - 1).start()
                if n >= 2:
                    arrived(mine(n - 2, across, 0), put_sem.at[n - 2, 2])
                    arrived(mine(n - 2, across, 1), put_sem.at[n - 2, 3])
            for n in range(shared, n_parts):
                arrived(mine(n), get_sem.at[n])

        loads[5].wait()
        turn(raw_skip.at[0:width], w_skip.at[0], 0)
        turn(raw_skip.at[width : 2 * width], w_skip.at[1], 0)
        for copy in warm:
            copy.wait()
        for s in range(samples):
            hub[s, 0] = raw_warm[0, s].T
            hub[s, SLOTS] = raw_warm[1, s].T
            x_t[s, 0] = x_ref[s]
        w_in[...] = jnp.zeros_like(w_in)
        w_in[:, 0 : win_ref.shape[0]] = win_ref[...].T

        t = Scratch()
        t.qkv, t.o, t.act, t.s, t.p = s_qkv, s_o, s_act, s_s, s_p
        steps_a, steps_b = steps - 1 - pair, steps - pair
        count = jnp.where(first_half, steps_a, steps_b)
        chained = jnp.where(first_half, pair > 0, pair < last_pair)
        chains = jnp.where(first_half, pair < last_pair, pair > 0)
        chain_count = jnp.where(first_half, steps - 3 - pair, steps_b)

        def chain(k, s):
            slot = lax.rem(k + 1, SLOTS)
            return remote(outs.at[s, lax.rem(k, 2)], hub.at[s, slot], csend_sem.at[s, lax.rem(k, 2)], crecv_sem.at[s, slot], chain_to)

        def skip(k, s):
            slot = lax.rem(k + 1, SLOTS)
            return remote(outs.at[s, lax.rem(k, 2)], hub.at[s, SLOTS + slot], ssend_sem.at[s, lax.rem(k, 2)], srecv_sem.at[s, slot], peer)

        def latent(k, s):
            slot = lax.rem(k + 1, 2)
            return remote(x_t.at[s, slot], x_t.at[s, slot], xsend_sem.at[s, slot], xrecv_sem.at[s, slot], peer)

        def tell(n, s):
            return remote(x_end.at[s], x_end.at[s], esend_sem.at[s, n], erecv_sem.at[s], {"data": group, "stage": n})

        def mods_at(k):
            return all_mod[pl.ds(pl.multiple_of(k * mod_rows, 8), mod_rows)]

        for half in range(2):
            spread(mods_at(0), half, mod_b.at[0])

        def step(m, _):
            k, s = m // samples, lax.rem(m, samples)
            slot, at = lax.rem(k, SLOTS), lax.rem(k, 2)

            @pl.when(jnp.logical_and(k > 0, chained))
            def _():
                arrived(hub.at[s, slot], crecv_sem.at[s, slot])

            @pl.when(jnp.logical_and(first_half, pair == 0))
            def _():
                @pl.when(k > 0)
                def _():
                    arrived(x_t.at[s, at], xrecv_sem.at[s, at])

                fill = jnp.zeros((CHUNK - channels, x_t.shape[3]), BF16)
                x_pad = jnp.concatenate([x_t[s, at].astype(BF16), fill], axis=0)
                for row in range(0, width, CHUNK):
                    h_ref[row : row + CHUNK] = product(w_in[row : row + CHUNK], x_pad)

            @pl.when(jnp.logical_and(first_half, pair > 0))
            def _():
                h_ref[...] = hub[s, slot].astype(F32)

            @pl.when(second_half)
            def _():
                @pl.when(k > 0)
                def _():
                    arrived(hub.at[s, SLOTS + slot], srecv_sem.at[s, slot])

                main = jnp.where(jnp.logical_and(k > 0, pair == last_pair), SLOTS + slot, slot)
                for row in range(0, width, CHUNK):
                    rows = slice(row, row + CHUNK)
                    h_ref[rows] = product(w_skip[1, rows], hub[s, SLOTS + slot]) + product(w_skip[0, rows], hub[s, main])

                @pl.when(k + SLOTS < count)
                def _():
                    pl.semaphore_signal(scredit_sem.at[s], inc=1, device_id=peer, device_id_type=mesh_ids)

            @pl.when(jnp.logical_and(chained, k + SLOTS < count))
            def _():
                pl.semaphore_signal(ccredit_sem.at[s], inc=1, device_id=chain_from, device_id_type=mesh_ids)

            @pl.when(k > 1)
            def _():
                @pl.when(first_half)
                def _():
                    skip(k - 2, s).wait_send()

                @pl.when(chains)
                def _():
                    chain(k - 2, s).wait_send()

            block(
                h_ref, mod_b.at[at], all_w, outs.at[s, at], t, heads,
                lambda: spread(mods_at(jnp.minimum(k + 1, steps - 1)), s, mod_b.at[1 - at]),
            )

            @pl.when(jnp.logical_and(chains, k < chain_count))
            def _():
                @pl.when(k + 1 >= SLOTS)
                def _():
                    pl.semaphore_wait(ccredit_sem.at[s], 1)

                chain(k, s).start()

            @pl.when(first_half)
            def _():
                @pl.when(k + 1 >= SLOTS)
                def _():
                    pl.semaphore_wait(scredit_sem.at[s], 1)

                skip(k, s).start()

            @pl.when(jnp.logical_and(second_half, pair == 0))
            def _():
                @pl.when(k > 1)
                def _():
                    latent(k - 2, s).wait_send()

                noise = product(wout_ref[...], outs[s, at])
                x_new = keep_ref[k] * x_t[s, at] + noise_ref[k] * noise
                x_t[s, 1 - at] = x_new

                @pl.when(k < steps - 2)
                def _():
                    latent(k, s).start()

                @pl.when(k == steps - 1)
                def _():
                    x_end[s] = x_new
                    for n in range(stages):

                        @pl.when(n != me)
                        def _():
                            tell(n, s).start()

            return 0

        lax.fori_loop(0, count * samples, step, 0)

        for s in range(samples):
            for back in (2, 1):

                @pl.when(first_half)
                def _():
                    skip(count - back, s).wait_send()

                @pl.when(jnp.logical_and(second_half, chains))
                def _():
                    chain(count - back, s).wait_send()

        for n in range(n_parts):

            @pl.when(beside)
            def _():
                hand(n).wait_send()

            @pl.when(away)
            def _():
                leave(n).wait_send()

            if n < shared:

                @pl.when(jnp.logical_not(is_local))
                def _():
                    for copy in (to_x(n), to_y(n), on_y(n), on_x(n)):
                        copy.wait_send()

        holder = jnp.logical_and(second_half, pair == 0)
        for s in range(samples):

            @pl.when(holder)
            def _():
                for n in range(stages):

                    @pl.when(n != me)
                    def _():
                        tell(n, s).wait_send()

            @pl.when(jnp.logical_not(holder))
            def _():
                arrived(x_end.at[s], erecv_sem.at[s])

            out_ref[s] = x_end[s]

    def local_run(x_init, h_warm, skip_warm, w_in, w_out, w_qkv, w_o, w_up, w_down, w_skip, ada_mods, keep, noise):
        batch, tokens, channels = x_init.shape
        width, ff = w_up.shape[1], w_up.shape[2]
        heads = w_o.shape[1]
        steps = ada_mods.shape[0]
        rows = 4 * width + 2 * ff
        mod_rows = 6 * width // 128
        any_ = pl.BlockSpec(memory_space=pl.ANY)
        vmem = pl.BlockSpec(memory_space=pltpu.VMEM)
        smem = pl.BlockSpec(memory_space=pltpu.SMEM)
        V = pltpu.VMEM
        D = pltpu.SemaphoreType.DMA
        R = pltpu.SemaphoreType.REGULAR
        parts = len(PIECES) + 1
        scratch = [
            V((width, 3 * width), BF16), V((width, width), BF16), V((width, ff), BF16), V((ff, width), BF16),
            V((rows, width), BF16), V((steps * mod_rows, 128), F32), V((rows, width), BF16), V((steps * mod_rows, 128), F32),
            V((2 * width, width), BF16), V((2, width, width), BF16), V((2, batch, tokens, width), BF16), V((width, CHUNK), BF16),
            V((batch, 2 * SLOTS, width, tokens), BF16), V((batch, 2, width, tokens), BF16),
            V((batch, 2, channels, tokens), F32), V((batch, channels, tokens), F32), V((width, tokens), F32),
            V((3 * width, tokens), BF16), V((width, tokens), BF16), V((ff, tokens), BF16),
            V((AHEAD + 1, tokens, tokens), F32), V((2, tokens, tokens), BF16), V((2, 6, width, 128), F32),
            D((6,)), D((2,)), D((parts,)), D((parts,)), D((parts, 4)), D((parts, 4)),
            D((batch, 2)), D((batch, SLOTS)), D((batch, 2)), D((batch, SLOTS)), D((batch, 2)), D((batch, 2)),
            D((batch, stages)), D((batch,)), R((batch,)), R((batch,)),
        ]
        call = pl.pallas_call(
            functools.partial(kernel, steps, heads),
            out_shape=jax.ShapeDtypeStruct((batch, channels, tokens), F32),
            in_specs=[vmem, any_, any_, vmem, vmem, any_, any_, any_, any_, any_, any_, smem, smem],
            out_specs=vmem,
            scratch_shapes=scratch,
            compiler_params=pltpu.CompilerParams(collective_id=0, has_side_effects=True, vmem_limit_bytes=60 * 2**20),
            name="staged_sampler",
        )
        made = call(
            x_init.swapaxes(1, 2), h_warm, skip_warm, w_in, w_out.T, w_qkv, w_o.reshape(1, width, width), w_up, w_down,
            w_skip, ada_mods.reshape(steps * mod_rows, 128), keep, noise,
        )
        return made.swapaxes(1, 2)

    in_specs = (P('data'), P(None, 'data'), P(None, 'data'), P(), P(), P('stage'), P('stage'), P('stage'), P('stage'), P(), P(None, 'stage'), P(), P())
    return jax.shard_map(local_run, mesh=mesh, in_specs=in_specs, out_specs=P('data'), check_vma=False)
```

```python
import functools
import math

import jax
import jax.numpy as jnp
from jax import lax
from jax.experimental import pallas as pl
from jax.experimental.pallas import tpu as pltpu
from jax.sharding import PartitionSpec as P

F32 = jnp.float32
BF16 = jnp.bfloat16
CHUNK = 256
CORES = 2
COLUMNS = 4
HEAD = 8
PIECES = (4, 8, 8, 8, 8, 7, 5)
FIRST = 1
SLOTS = 4
EPS = 1e-6
AHEAD = 5
UP_AHEAD = 2
DOWN_BEHIND = 1
TANH_A = math.sqrt(2.0 / math.pi)
TANH_B = TANH_A * 0.044715


def product(lhs, rhs):
    return jnp.dot(lhs, rhs, preferred_element_type=F32)


def norm_mod(h_ref, scale, shift):
    width = h_ref.shape[0]

    def total(term):
        sums = [None] * 4
        for n, row in enumerate(range(0, width, 8)):
            v = term(h_ref[row : row + 8, :])
            sums[n % 4] = v if sums[n % 4] is None else sums[n % 4] + v
        return jnp.sum((sums[0] + sums[1]) + (sums[2] + sums[3]), axis=0, keepdims=True) * (1.0 / width)

    mean = total(lambda v: v)
    rate = lax.rsqrt(total(lambda v: (v - mean) * (v - mean)) + EPS)
    rows = [slice(row, row + 16) for row in range(0, width, 16)]
    return jnp.concatenate(
        [(((h_ref[r, :] - mean) * rate) * wide(scale[r]) + wide(shift[r])).astype(BF16) for r in rows], axis=0
    )


def gelu(x):
    return (x * (0.5 + 0.5 * jnp.tanh(x * (TANH_A + TANH_B * (x * x))))).astype(BF16)


def softmax(s, scale):
    m = jnp.max(s, axis=0, keepdims=True)
    p = jnp.exp2((s - m) * (scale * math.log2(math.e)))
    return p.astype(BF16), 1.0 / jnp.sum(p, axis=0, keepdims=True)


def wide(cols):
    return jnp.concatenate([cols, cols], axis=1)


def spread(mods, half, dst):
    rows = dst.shape[1] // 128
    cols = mods.T
    cols = jnp.where(half == 0, cols[:, 0 : 3 * rows], cols[:, 3 * rows : 6 * rows])
    for v in range(3):
        for n in range(rows):
            col = cols[:, rows * v + n : rows * v + n + 1]
            if v == 1:
                col = 1.0 + col
            dst[3 * half + v, 128 * n : 128 * (n + 1), :] = jnp.broadcast_to(col, (128, 128))


def block(h_ref, mod, w, out, t, heads, extra):
    width, tokens = h_ref.shape
    dim = width // heads
    per_group = CHUNK // dim
    groups = heads // per_group
    row_o, row_up = 3 * width, 4 * width
    ff = (w.shape[0] - row_up) // 2
    row_down = row_up + ff

    u = norm_mod(h_ref, mod[1], mod[0])
    for row, size in [(width + CHUNK * g, CHUNK) if n == 0 else (CHUNK * g, CHUNK) for g in range(groups) for n in range(2)] + [
        (2 * width, width)
    ]:
        t.qkv[row : row + size] = product(w[row : row + size], u).astype(BF16)

    zero = jnp.zeros((dim, tokens), BF16)
    keys, rate = {}, {}

    def scores(hd):
        g, j = divmod(hd, per_group)
        if g not in keys:
            keys[g] = t.qkv[width + CHUNK * g : width + CHUNK * (g + 1), :].T
        query = t.qkv[dim * hd : dim * (hd + 1), :]
        padded = jnp.concatenate([query if m == j else zero for m in range(per_group)], axis=0)
        t.s[hd % (AHEAD + 1)] = product(keys[g], padded)

    def probs(hd):
        t.p[hd % 2], rate[hd] = softmax(t.s[hd % (AHEAD + 1)], 1.0 / math.sqrt(dim))

    def values(hd):
        row = dim * hd
        v = product(t.qkv[2 * width + row : 2 * width + row + dim, :], t.p[hd % 2])
        t.o[row : row + dim, :] = (v * rate[hd]).astype(BF16)

    for n in range(AHEAD):
        scores(n)
    for n in range(heads):
        if n + AHEAD < heads:
            scores(n + AHEAD)
        probs(n)
        values(n)

    for row in range(0, width, CHUNK):
        rows = slice(row, row + CHUNK)
        h_ref[rows] = h_ref[rows] + wide(mod[2, rows]) * product(w[row_o + row : row_o + row + CHUNK], t.o[...])
    u = norm_mod(h_ref, mod[4], mod[3])
    chunks = ff // CHUNK
    held, total = {}, [None] * (width // CHUNK)

    def up(n):
        held[n] = product(w[row_up + CHUNK * n : row_up + CHUNK * (n + 1)], u)

    def down(n):
        at, col = divmod(CHUNK * n, width)
        for q in range(len(total)):
            row = row_down + width * at + CHUNK * q
            part = product(w[row : row + CHUNK, col : col + CHUNK], t.act[CHUNK * n : CHUNK * (n + 1), :])
            total[q] = part if total[q] is None else total[q] + part

    for n in range(UP_AHEAD):
        up(n)
    for n in range(chunks):
        if n + UP_AHEAD < chunks:
            up(n + UP_AHEAD)
        t.act[CHUNK * n : CHUNK * (n + 1), :] = gelu(held.pop(n))
        if n == 0:
            extra()
        if n >= DOWN_BEHIND:
            down(n - DOWN_BEHIND)
    for n in range(chunks - DOWN_BEHIND, chunks):
        down(n)
    for q, v in enumerate(total):
        rows = slice(CHUNK * q, CHUNK * (q + 1))
        out[rows] = (h_ref[rows] + wide(mod[5, rows]) * v).astype(BF16)


class Scratch:
    pass


def solution(mesh):
    stages = mesh.shape["stage"]
    chips = stages // CORES
    side = math.isqrt(mesh.shape["data"])
    if side * side != mesh.shape["data"] or side % 2:
        raise ValueError("data axis")

    def kernel(
        steps, heads,
        x_ref, hwarm_ref, swarm_ref, win_ref, wout_ref, wqkv_ref, wo_ref, wup_ref, wdown_ref, wskip_ref, mods_ref,
        keep_ref, noise_ref,
        out_ref,
        raw_qkv, raw_o, raw_up, raw_down, home_w, home_mod, all_w, all_mod,
        raw_skip, w_skip, raw_warm, w_in,
        hub, outs, x_t, x_end, h_ref, s_qkv, s_o, s_act, s_s, s_p, mod_b,
        load_sem, warm_sem, hsend_sem, get_sem, send_sem, put_sem,
        csend_sem, crecv_sem, ssend_sem, srecv_sem, xsend_sem, xrecv_sem, esend_sem, erecv_sem,
        ccredit_sem, scredit_sem,
    ):
        me = lax.axis_index("stage")
        group = lax.axis_index("data")
        chip, core = me // CORES, lax.rem(me, CORES)
        pair = lax.rem(chips + FIRST - chip, chips)
        first_half, second_half = core == 0, core == 1
        stage = jnp.where(first_half, pair, stages - 1 - pair)
        last_pair = chips - 1
        samples, channels = x_ref.shape[0], x_ref.shape[1]
        width = raw_o.shape[0]
        n_parts = len(PIECES) + 2
        mod_rows = 6 * width // 128
        mesh_ids = pl.DeviceIdType.MESH

        odd_x, odd_y = lax.rem(group // side, 2), lax.rem(group, 2)
        column = 2 * odd_x + odd_y
        next_x = {"data": group + side * (1 - 2 * odd_x), "stage": me}
        next_y = {"data": group + 1 - 2 * odd_y, "stage": me}
        beside_x, beside_y = 2 * (1 - odd_x) + odd_y, 2 * odd_x + 1 - odd_y
        across = 2 * (1 - odd_x) + 1 - odd_y

        def device(chip_, core_):
            return {"data": group, "stage": chip_ * CORES + core_}

        peer = device(chip, 1 - core)
        chain_to = device(jnp.where(first_half, lax.rem(chip + chips - 1, chips), lax.rem(chip + 1, chips)), core)
        chain_from = device(jnp.where(first_half, lax.rem(chip + 1, chips), lax.rem(chip + chips - 1, chips)), core)

        def remote(src, dst, send, recv, to):
            return pltpu.make_async_remote_copy(
                src_ref=src, dst_ref=dst, send_sem=send, recv_sem=recv, device_id=to, device_id_type=mesh_ids
            )

        def arrived(ref, sem):
            pltpu.make_async_copy(ref, ref, sem).wait()

        barrier = pltpu.get_barrier_semaphore()
        for n in range(1, stages):
            pl.semaphore_signal(
                barrier, inc=1, device_id={"data": group, "stage": lax.rem(me + n, stages)}, device_id_type=mesh_ids
            )
        for beyond in (next_x, next_y):
            pl.semaphore_signal(barrier, inc=1, device_id=beyond, device_id_type=mesh_ids)

        raws = [raw_qkv, raw_o, raw_up, raw_down]
        homes = [wqkv_ref, wo_ref, wup_ref, wdown_ref]
        loads = [pltpu.make_async_copy(src.at[0], dst, load_sem.at[n]) for n, (src, dst) in enumerate(zip(homes, raws))]
        loads.append(pltpu.make_async_copy(mods_ref, home_mod, load_sem.at[4]))
        loads.append(pltpu.make_async_copy(wskip_ref.at[last_pair - pair], raw_skip, load_sem.at[5]))
        chain_warm = jnp.maximum(stage - 1, 0)
        warm = [
            pltpu.make_async_copy(hwarm_ref.at[chain_warm], raw_warm.at[0], warm_sem.at[0]),
            pltpu.make_async_copy(swarm_ref.at[pair], raw_warm.at[1], warm_sem.at[1]),
        ]
        for n in (4, 0, 1, 2, 3, 5):
            loads[n].start()
        for copy in warm:
            copy.start()

        def turn(src, dst, row):
            for at in range(0, src.shape[1], CHUNK):
                dst[row + at : row + at + CHUNK, :] = src[:, at : at + CHUNK].T

        home_pair = jnp.minimum(me, stages - 1 - me)
        goal_chip, goal_core = lax.rem(chips + FIRST - home_pair, chips), jnp.where(me < chips, 0, 1)
        goal = device(goal_chip, goal_core)
        here = jnp.logical_and(goal_chip == chip, goal_core == core)
        beside = jnp.logical_and(goal_chip == chip, goal_core != core)
        away = goal_chip != chip
        is_local = stage // CORES == chip
        shared, tail = n_parts - 2, n_parts - 1
        ends = [home_w.shape[0] * sum(PIECES[:n]) // sum(PIECES) for n in range(tail)]
        head_rows = HEAD * mod_rows

        def part(n, ref_w, ref_mod, column_=None, half=None):
            is_mod = n in (0, tail)
            if is_mod:
                size, at = (head_rows, 0) if n == 0 else (ref_mod.shape[0] - head_rows, head_rows)
            else:
                size, at = ends[n] - ends[n - 1], ends[n - 1]
            if column_ is not None:
                size //= COLUMNS
                at = at + column_ * size
            if half is not None:
                size //= 2
                at = at + half * size
            rows = pl.ds(at if isinstance(at, int) else pl.multiple_of(at, 8 if is_mod else 16), size)
            return (ref_mod if is_mod else ref_w).at[rows]

        def home(n, column_=None):
            return part(n, home_w, home_mod, column_)

        def mine(n, column_=None, half=None):
            return part(n, all_w, all_mod, column_, half)

        def stay(n):
            return pltpu.make_async_copy(home(n), mine(n), get_sem.at[n])

        def hand(n):
            return remote(home(n), mine(n), hsend_sem.at[n], get_sem.at[n], peer)

        def leave(n):
            which = column if n < shared else None
            return remote(home(n, which), mine(n, which), hsend_sem.at[n], get_sem.at[n], goal)

        def send_now(n):
            @pl.when(here)
            def _():
                stay(n).start()

            @pl.when(beside)
            def _():
                hand(n).start()

            @pl.when(away)
            def _():
                leave(n).start()

        loads[4].wait()
        sent, row = -1, 0
        jobs = [(0, raw_qkv), (1, raw_o), (2, raw_up)]
        jobs += [(3, raw_down.at[width * n : width * (n + 1)]) for n in range(raw_down.shape[0] // width)]
        ready = -1
        for load, src in jobs:
            if load > ready:
                loads[load].wait()
                ready = load
            for col in range(0, src.shape[1], width):
                turn(src.at[:, col : col + width], home_w, row)
                row += width
                while sent + 1 < tail and ends[sent + 1] <= row:
                    if sent < 0:
                        pl.semaphore_wait(barrier, stages + 1)
                    sent += 1
                    send_now(sent)
        send_now(tail)

        def to_x(n):
            return remote(mine(n, column), mine(n, column), send_sem.at[n, 0], put_sem.at[n, 0], next_x)

        def to_y(n):
            return remote(mine(n, column), mine(n, column), send_sem.at[n, 1], put_sem.at[n, 1], next_y)

        def on_y(n):
            return remote(mine(n, beside_x, 0), mine(n, beside_x, 0), send_sem.at[n, 2], put_sem.at[n, 2], next_y)

        def on_x(n):
            return remote(mine(n, beside_y, 1), mine(n, beside_y, 1), send_sem.at[n, 3], put_sem.at[n, 3], next_x)

        def mods_at(k):
            return all_mod[pl.ds(pl.multiple_of(k * mod_rows, 8), mod_rows)]

        def prepare():
            loads[5].wait()
            turn(raw_skip.at[0:width], w_skip.at[0], 0)
            turn(raw_skip.at[width : 2 * width], w_skip.at[1], 0)
            for copy in warm:
                copy.wait()
            for s in range(samples):
                hub[s, 0] = raw_warm[0, s].T
                hub[s, SLOTS] = raw_warm[1, s].T
                x_t[s, 0] = x_ref[s]
            w_in[...] = jnp.zeros_like(w_in)
            w_in[:, 0 : win_ref.shape[0]] = win_ref[...].T
            for half in range(2):
                spread(mods_at(0), half, mod_b.at[0])

        @pl.when(is_local)
        def _():
            arrived(mine(0), get_sem.at[0])
            prepare()
            for n in range(1, tail):
                arrived(mine(n), get_sem.at[n])

        @pl.when(jnp.logical_not(is_local))
        def _():
            for n in range(shared + 2):
                if n < shared:
                    arrived(mine(n, column), get_sem.at[n])
                    to_x(n).start()
                    to_y(n).start()
                if 1 <= n <= shared:
                    arrived(mine(n - 1, beside_x), put_sem.at[n - 1, 0])
                    on_y(n - 1).start()
                    arrived(mine(n - 1, beside_y), put_sem.at[n - 1, 1])
                    on_x(n - 1).start()
                if n >= 2:
                    arrived(mine(n - 2, across, 0), put_sem.at[n - 2, 2])
                    arrived(mine(n - 2, across, 1), put_sem.at[n - 2, 3])
                if n == 2:
                    prepare()
            for n in range(shared, tail):
                arrived(mine(n), get_sem.at[n])

        t = Scratch()
        t.qkv, t.o, t.act, t.s, t.p = s_qkv, s_o, s_act, s_s, s_p
        steps_a, steps_b = steps - 1 - pair, steps - pair
        count = jnp.where(first_half, steps_a, steps_b)
        chained = jnp.where(first_half, pair > 0, pair < last_pair)
        chains = jnp.where(first_half, pair < last_pair, pair > 0)
        chain_count = jnp.where(first_half, steps - 3 - pair, steps_b)

        def chain(k, s):
            slot = lax.rem(k + 1, SLOTS)
            return remote(outs.at[s, lax.rem(k, 2)], hub.at[s, slot], csend_sem.at[s, lax.rem(k, 2)], crecv_sem.at[s, slot], chain_to)

        def skip(k, s):
            slot = lax.rem(k + 1, SLOTS)
            return remote(outs.at[s, lax.rem(k, 2)], hub.at[s, SLOTS + slot], ssend_sem.at[s, lax.rem(k, 2)], srecv_sem.at[s, slot], peer)

        def latent(k, s):
            slot = lax.rem(k + 1, 2)
            return remote(x_t.at[s, slot], x_t.at[s, slot], xsend_sem.at[s, slot], xrecv_sem.at[s, slot], peer)

        def tell(n, s):
            return remote(x_end.at[s], x_end.at[s], esend_sem.at[s, n], erecv_sem.at[s], {"data": group, "stage": n})

        def step(m, _):
            k, s = m // samples, lax.rem(m, samples)
            slot, at = lax.rem(k, SLOTS), lax.rem(k, 2)

            @pl.when(m == HEAD // 2 * samples)
            def _():
                arrived(mine(tail), get_sem.at[tail])

            @pl.when(jnp.logical_and(k > 0, chained))
            def _():
                arrived(hub.at[s, slot], crecv_sem.at[s, slot])

            @pl.when(jnp.logical_and(first_half, pair == 0))
            def _():
                @pl.when(k > 0)
                def _():
                    arrived(x_t.at[s, at], xrecv_sem.at[s, at])

                fill = jnp.zeros((CHUNK - channels, x_t.shape[3]), BF16)
                x_pad = jnp.concatenate([x_t[s, at].astype(BF16), fill], axis=0)
                for row in range(0, width, CHUNK):
                    h_ref[row : row + CHUNK] = product(w_in[row : row + CHUNK], x_pad)

            @pl.when(jnp.logical_and(first_half, pair > 0))
            def _():
                h_ref[...] = hub[s, slot].astype(F32)

            @pl.when(second_half)
            def _():
                @pl.when(k > 0)
                def _():
                    arrived(hub.at[s, SLOTS + slot], srecv_sem.at[s, slot])

                main = jnp.where(jnp.logical_and(k > 0, pair == last_pair), SLOTS + slot, slot)
                for row in range(0, width, CHUNK):
                    rows = slice(row, row + CHUNK)
                    h_ref[rows] = product(w_skip[1, rows], hub[s, SLOTS + slot]) + product(w_skip[0, rows], hub[s, main])

                @pl.when(k + SLOTS < count)
                def _():
                    pl.semaphore_signal(scredit_sem.at[s], inc=1, device_id=peer, device_id_type=mesh_ids)

            @pl.when(jnp.logical_and(chained, k + SLOTS < count))
            def _():
                pl.semaphore_signal(ccredit_sem.at[s], inc=1, device_id=chain_from, device_id_type=mesh_ids)

            @pl.when(k > 1)
            def _():
                @pl.when(first_half)
                def _():
                    skip(k - 2, s).wait_send()

                @pl.when(chains)
                def _():
                    chain(k - 2, s).wait_send()

            block(
                h_ref, mod_b.at[at], all_w, outs.at[s, at], t, heads,
                lambda: spread(mods_at(jnp.minimum(k + 1, steps - 1)), s, mod_b.at[1 - at]),
            )

            @pl.when(jnp.logical_and(chains, k < chain_count))
            def _():
                @pl.when(k + 1 >= SLOTS)
                def _():
                    pl.semaphore_wait(ccredit_sem.at[s], 1)

                chain(k, s).start()

            @pl.when(first_half)
            def _():
                @pl.when(k + 1 >= SLOTS)
                def _():
                    pl.semaphore_wait(scredit_sem.at[s], 1)

                skip(k, s).start()

            @pl.when(jnp.logical_and(second_half, pair == 0))
            def _():
                @pl.when(k > 1)
                def _():
                    latent(k - 2, s).wait_send()

                noise = product(wout_ref[...], outs[s, at])
                x_new = keep_ref[k] * x_t[s, at] + noise_ref[k] * noise
                x_t[s, 1 - at] = x_new

                @pl.when(k < steps - 2)
                def _():
                    latent(k, s).start()

                @pl.when(k == steps - 1)
                def _():
                    x_end[s] = x_new
                    for n in range(stages):

                        @pl.when(n != me)
                        def _():
                            tell(n, s).start()

            return 0

        lax.fori_loop(0, count * samples, step, 0)

        for s in range(samples):
            for back in (2, 1):

                @pl.when(first_half)
                def _():
                    skip(count - back, s).wait_send()

                @pl.when(jnp.logical_and(second_half, chains))
                def _():
                    chain(count - back, s).wait_send()

        for n in range(n_parts):

            @pl.when(beside)
            def _():
                hand(n).wait_send()

            @pl.when(away)
            def _():
                leave(n).wait_send()

            if n < shared:

                @pl.when(jnp.logical_not(is_local))
                def _():
                    for copy in (to_x(n), to_y(n), on_y(n), on_x(n)):
                        copy.wait_send()

        holder = jnp.logical_and(second_half, pair == 0)
        for s in range(samples):

            @pl.when(holder)
            def _():
                for n in range(stages):

                    @pl.when(n != me)
                    def _():
                        tell(n, s).wait_send()

            @pl.when(jnp.logical_not(holder))
            def _():
                arrived(x_end.at[s], erecv_sem.at[s])

            out_ref[s] = x_end[s]

    def local_run(x_init, h_warm, skip_warm, w_in, w_out, w_qkv, w_o, w_up, w_down, w_skip, ada_mods, keep, noise):
        batch, tokens, channels = x_init.shape
        width, ff = w_up.shape[1], w_up.shape[2]
        heads = w_o.shape[1]
        steps = ada_mods.shape[0]
        rows = 4 * width + 2 * ff
        mod_rows = 6 * width // 128
        any_ = pl.BlockSpec(memory_space=pl.ANY)
        vmem = pl.BlockSpec(memory_space=pltpu.VMEM)
        smem = pl.BlockSpec(memory_space=pltpu.SMEM)
        V = pltpu.VMEM
        D = pltpu.SemaphoreType.DMA
        R = pltpu.SemaphoreType.REGULAR
        parts = len(PIECES) + 2
        scratch = [
            V((width, 3 * width), BF16), V((width, width), BF16), V((width, ff), BF16), V((ff, width), BF16),
            V((rows, width), BF16), V((steps * mod_rows, 128), F32), V((rows, width), BF16), V((steps * mod_rows, 128), F32),
            V((2 * width, width), BF16), V((2, width, width), BF16), V((2, batch, tokens, width), BF16), V((width, CHUNK), BF16),
            V((batch, 2 * SLOTS, width, tokens), BF16), V((batch, 2, width, tokens), BF16),
            V((batch, 2, channels, tokens), F32), V((batch, channels, tokens), F32), V((width, tokens), F32),
            V((3 * width, tokens), BF16), V((width, tokens), BF16), V((ff, tokens), BF16),
            V((AHEAD + 1, tokens, tokens), F32), V((2, tokens, tokens), BF16), V((2, 6, width, 128), F32),
            D((6,)), D((2,)), D((parts,)), D((parts,)), D((parts, 4)), D((parts, 4)),
            D((batch, 2)), D((batch, SLOTS)), D((batch, 2)), D((batch, SLOTS)), D((batch, 2)), D((batch, 2)),
            D((batch, stages)), D((batch,)), R((batch,)), R((batch,)),
        ]
        call = pl.pallas_call(
            functools.partial(kernel, steps, heads),
            out_shape=jax.ShapeDtypeStruct((batch, channels, tokens), F32),
            in_specs=[vmem, any_, any_, vmem, vmem, any_, any_, any_, any_, any_, any_, smem, smem],
            out_specs=vmem,
            scratch_shapes=scratch,
            compiler_params=pltpu.CompilerParams(collective_id=0, has_side_effects=True, vmem_limit_bytes=60 * 2**20),
            name="staged_sampler",
        )
        made = call(
            x_init.swapaxes(1, 2), h_warm, skip_warm, w_in, w_out.T, w_qkv, w_o.reshape(1, width, width), w_up, w_down,
            w_skip, ada_mods.reshape(steps * mod_rows, 128), keep, noise,
        )
        return made.swapaxes(1, 2)

    in_specs = (P('data'), P(None, 'data'), P(None, 'data'), P(), P(), P('stage'), P('stage'), P('stage'), P('stage'), P(), P(None, 'stage'), P(), P())
    return jax.shard_map(local_run, mesh=mesh, in_specs=in_specs, out_specs=P('data'), check_vma=False)
```

```python
import functools
import math

import jax
import jax.numpy as jnp
from jax import lax
from jax.experimental import pallas as pl
from jax.experimental.pallas import tpu as pltpu
from jax.sharding import PartitionSpec as P

F32 = jnp.float32
BF16 = jnp.bfloat16
CHUNK = 256
CORES = 2
COLUMNS = 4
HEAD = 8
PIECES = (4, 8, 8, 8, 8, 7, 5)
FIRST = 1
SLOTS = 4
EPS = 1e-6
AHEAD = 5
UP_AHEAD = 2
DOWN_BEHIND = 1
TANH_A = math.sqrt(2.0 / math.pi)
TANH_B = TANH_A * 0.044715


def product(lhs, rhs):
    return jnp.dot(lhs, rhs, preferred_element_type=F32)


def norm_mod(h_ref, scale, shift):
    width = h_ref.shape[0]

    def total(term):
        sums = [None] * 4
        for n, row in enumerate(range(0, width, 8)):
            v = term(h_ref[row : row + 8, :])
            sums[n % 4] = v if sums[n % 4] is None else sums[n % 4] + v
        return jnp.sum((sums[0] + sums[1]) + (sums[2] + sums[3]), axis=0, keepdims=True) * (1.0 / width)

    mean = total(lambda v: v)
    rate = lax.rsqrt(total(lambda v: (v - mean) * (v - mean)) + EPS)
    rows = [slice(row, row + 16) for row in range(0, width, 16)]
    return jnp.concatenate(
        [(((h_ref[r, :] - mean) * rate) * wide(scale[r]) + wide(shift[r])).astype(BF16) for r in rows], axis=0
    )


def gelu(x):
    return (x * (0.5 + 0.5 * jnp.tanh(x * (TANH_A + TANH_B * (x * x))))).astype(BF16)


def softmax(s, scale):
    m = jnp.max(s, axis=0, keepdims=True)
    p = jnp.exp2((s - m) * (scale * math.log2(math.e)))
    return p.astype(BF16), 1.0 / jnp.sum(p, axis=0, keepdims=True)


def wide(cols):
    return jnp.concatenate([cols, cols], axis=1)


def spread(mods, half, dst):
    rows = dst.shape[1] // 128
    cols = mods.T
    cols = jnp.where(half == 0, cols[:, 0 : 3 * rows], cols[:, 3 * rows : 6 * rows])
    for v in range(3):
        for n in range(rows):
            col = cols[:, rows * v + n : rows * v + n + 1]
            if v == 1:
                col = 1.0 + col
            dst[3 * half + v, 128 * n : 128 * (n + 1), :] = jnp.broadcast_to(col, (128, 128))


def block(h_ref, mod, w, out, t, heads, extra):
    width, tokens = h_ref.shape
    dim = width // heads
    per_group = CHUNK // dim
    groups = heads // per_group
    row_o, row_up = 3 * width, 4 * width
    ff = (w.shape[0] - row_up) // 2
    row_down = row_up + ff

    u = norm_mod(h_ref, mod[1], mod[0])
    for row, size in [(width + CHUNK * g, CHUNK) if n == 0 else (CHUNK * g, CHUNK) for g in range(groups) for n in range(2)] + [
        (2 * width, width)
    ]:
        t.qkv[row : row + size] = product(w[row : row + size], u).astype(BF16)

    zero = jnp.zeros((dim, tokens), BF16)
    keys, rate = {}, {}

    def scores(hd):
        g, j = divmod(hd, per_group)
        if g not in keys:
            keys[g] = t.qkv[width + CHUNK * g : width + CHUNK * (g + 1), :].T
        query = t.qkv[dim * hd : dim * (hd + 1), :]
        padded = jnp.concatenate([query if m == j else zero for m in range(per_group)], axis=0)
        t.s[hd % (AHEAD + 1)] = product(keys[g], padded)

    def probs(hd):
        t.p[hd % 2], rate[hd] = softmax(t.s[hd % (AHEAD + 1)], 1.0 / math.sqrt(dim))

    def values(hd):
        row = dim * hd
        v = product(t.qkv[2 * width + row : 2 * width + row + dim, :], t.p[hd % 2])
        t.o[row : row + dim, :] = (v * rate[hd]).astype(BF16)

    for n in range(AHEAD):
        scores(n)
    for n in range(heads):
        if n + AHEAD < heads:
            scores(n + AHEAD)
        probs(n)
        values(n)

    for row in range(0, width, CHUNK):
        rows = slice(row, row + CHUNK)
        h_ref[rows] = h_ref[rows] + wide(mod[2, rows]) * product(w[row_o + row : row_o + row + CHUNK], t.o[...])
    u = norm_mod(h_ref, mod[4], mod[3])
    chunks = ff // CHUNK
    held, total = {}, [None] * (width // CHUNK)

    def up(n):
        held[n] = product(w[row_up + CHUNK * n : row_up + CHUNK * (n + 1)], u)

    def down(n):
        at, col = divmod(CHUNK * n, width)
        for q in range(len(total)):
            row = row_down + width * at + CHUNK * q
            part = product(w[row : row + CHUNK, col : col + CHUNK], t.act[CHUNK * n : CHUNK * (n + 1), :])
            total[q] = part if total[q] is None else total[q] + part

    for n in range(UP_AHEAD):
        up(n)
    for n in range(chunks):
        if n + UP_AHEAD < chunks:
            up(n + UP_AHEAD)
        t.act[CHUNK * n : CHUNK * (n + 1), :] = gelu(held.pop(n))
        if n == 0:
            extra()
        if n >= DOWN_BEHIND:
            down(n - DOWN_BEHIND)
    for n in range(chunks - DOWN_BEHIND, chunks):
        down(n)
    for q, v in enumerate(total):
        rows = slice(CHUNK * q, CHUNK * (q + 1))
        out[rows] = (h_ref[rows] + wide(mod[5, rows]) * v).astype(BF16)


class Scratch:
    pass


def solution(mesh):
    stages = mesh.shape["stage"]
    chips = stages // CORES
    side = math.isqrt(mesh.shape["data"])
    if side * side != mesh.shape["data"] or side % 2:
        raise ValueError("data axis")

    def kernel(
        steps, heads,
        x_ref, hwarm_ref, swarm_ref, win_ref, wout_ref, wqkv_ref, wo_ref, wup_ref, wdown_ref, wskip_ref, mods_ref,
        keep_ref, noise_ref,
        out_ref,
        raw_qkv, raw_o, raw_up, raw_down, home_w, home_mod, all_w, all_mod,
        raw_skip, w_skip, raw_warm, w_in,
        hub, outs, x_t, x_end, h_ref, s_qkv, s_o, s_act, s_s, s_p, mod_b,
        load_sem, warm_sem, hsend_sem, get_sem, send_sem, put_sem,
        csend_sem, crecv_sem, ssend_sem, srecv_sem, xsend_sem, xrecv_sem, esend_sem, erecv_sem,
        ccredit_sem, scredit_sem,
    ):
        me = lax.axis_index("stage")
        group = lax.axis_index("data")
        chip, core = me // CORES, lax.rem(me, CORES)
        pair = lax.rem(chips + FIRST - chip, chips)
        first_half, second_half = core == 0, core == 1
        stage = jnp.where(first_half, pair, stages - 1 - pair)
        last_pair = chips - 1
        samples, channels = x_ref.shape[0], x_ref.shape[1]
        width = raw_o.shape[0]
        n_parts = len(PIECES) + 2
        mod_rows = 6 * width // 128
        mesh_ids = pl.DeviceIdType.MESH

        odd_x, odd_y = lax.rem(group // side, 2), lax.rem(group, 2)
        column = 2 * odd_x + odd_y
        next_x = {"data": group + side * (1 - 2 * odd_x), "stage": me}
        next_y = {"data": group + 1 - 2 * odd_y, "stage": me}
        beside_x, beside_y = 2 * (1 - odd_x) + odd_y, 2 * odd_x + 1 - odd_y
        across = 2 * (1 - odd_x) + 1 - odd_y

        def device(chip_, core_):
            return {"data": group, "stage": chip_ * CORES + core_}

        peer = device(chip, 1 - core)
        chain_to = device(jnp.where(first_half, lax.rem(chip + chips - 1, chips), lax.rem(chip + 1, chips)), core)
        chain_from = device(jnp.where(first_half, lax.rem(chip + 1, chips), lax.rem(chip + chips - 1, chips)), core)

        def remote(src, dst, send, recv, to):
            return pltpu.make_async_remote_copy(
                src_ref=src, dst_ref=dst, send_sem=send, recv_sem=recv, device_id=to, device_id_type=mesh_ids
            )

        def arrived(ref, sem):
            pltpu.make_async_copy(ref, ref, sem).wait()

        barrier = pltpu.get_barrier_semaphore()
        for n in range(1, stages):
            pl.semaphore_signal(
                barrier, inc=1, device_id={"data": group, "stage": lax.rem(me + n, stages)}, device_id_type=mesh_ids
            )
        for beyond in (next_x, next_y):
            pl.semaphore_signal(barrier, inc=1, device_id=beyond, device_id_type=mesh_ids)

        raws = [raw_qkv, raw_o, raw_up, raw_down]
        homes = [wqkv_ref, wo_ref, wup_ref, wdown_ref]
        loads = [pltpu.make_async_copy(src.at[0], dst, load_sem.at[n]) for n, (src, dst) in enumerate(zip(homes, raws))]
        loads.append(pltpu.make_async_copy(mods_ref, home_mod, load_sem.at[4]))
        loads.append(pltpu.make_async_copy(wskip_ref.at[last_pair - pair], raw_skip, load_sem.at[5]))
        chain_warm = jnp.maximum(stage - 1, 0)
        warm = [
            pltpu.make_async_copy(hwarm_ref.at[chain_warm], raw_warm.at[0], warm_sem.at[0]),
            pltpu.make_async_copy(swarm_ref.at[pair], raw_warm.at[1], warm_sem.at[1]),
        ]
        for n in (4, 0, 1, 2, 3, 5):
            loads[n].start()
        for copy in warm:
            copy.start()

        def turn(src, dst, row):
            for at in range(0, src.shape[1], CHUNK):
                dst[row + at : row + at + CHUNK, :] = src[:, at : at + CHUNK].T

        home_pair = jnp.minimum(me, stages - 1 - me)
        goal_chip, goal_core = lax.rem(chips + FIRST - home_pair, chips), jnp.where(me < chips, 0, 1)
        goal = device(goal_chip, goal_core)
        here = jnp.logical_and(goal_chip == chip, goal_core == core)
        beside = jnp.logical_and(goal_chip == chip, goal_core != core)
        away = goal_chip != chip
        is_local = stage // CORES == chip
        shared, tail = n_parts - 2, n_parts - 1
        ends = [home_w.shape[0] * sum(PIECES[:n]) // sum(PIECES) for n in range(tail)]
        head_rows = HEAD * mod_rows

        def part(n, ref_w, ref_mod, column_=None, half=None):
            is_mod = n in (0, tail)
            if is_mod:
                size, at = (head_rows, 0) if n == 0 else (ref_mod.shape[0] - head_rows, head_rows)
            else:
                size, at = ends[n] - ends[n - 1], ends[n - 1]
            if column_ is not None:
                size //= COLUMNS
                at = at + column_ * size
            if half is not None:
                size //= 2
                at = at + half * size
            rows = pl.ds(at if isinstance(at, int) else pl.multiple_of(at, 8 if is_mod else 16), size)
            return (ref_mod if is_mod else ref_w).at[rows]

        def home(n, column_=None):
            return part(n, home_w, home_mod, column_)

        def mine(n, column_=None, half=None):
            return part(n, all_w, all_mod, column_, half)

        def stay(n):
            return pltpu.make_async_copy(home(n), mine(n), get_sem.at[n])

        def hand(n):
            return remote(home(n), mine(n), hsend_sem.at[n], get_sem.at[n], peer)

        def leave(n):
            which = column if n < shared else None
            return remote(home(n, which), mine(n, which), hsend_sem.at[n], get_sem.at[n], goal)

        def send_now(n):
            @pl.when(here)
            def _():
                stay(n).start()

            @pl.when(beside)
            def _():
                hand(n).start()

            @pl.when(away)
            def _():
                leave(n).start()

        loads[4].wait()
        sent, row = -1, 0
        jobs = [(0, raw_qkv), (1, raw_o), (2, raw_up)]
        jobs += [(3, raw_down.at[width * n : width * (n + 1)]) for n in range(raw_down.shape[0] // width)]
        ready = -1
        for load, src in jobs:
            if load > ready:
                loads[load].wait()
                ready = load
            for col in range(0, src.shape[1], width):
                turn(src.at[:, col : col + width], home_w, row)
                row += width
                while sent + 1 < tail and ends[sent + 1] <= row:
                    if sent < 0:
                        pl.semaphore_wait(barrier, stages + 1)
                    sent += 1
                    send_now(sent)
        send_now(tail)

        def to_x(n):
            return remote(mine(n, column), mine(n, column), send_sem.at[n, 0], put_sem.at[n, 0], next_x)

        def to_y(n):
            return remote(mine(n, column), mine(n, column), send_sem.at[n, 1], put_sem.at[n, 1], next_y)

        def on_y(n):
            return remote(mine(n, beside_x, 0), mine(n, beside_x, 0), send_sem.at[n, 2], put_sem.at[n, 2], next_y)

        def on_x(n):
            return remote(mine(n, beside_y, 1), mine(n, beside_y, 1), send_sem.at[n, 3], put_sem.at[n, 3], next_x)

        def mods_at(k):
            return all_mod[pl.ds(pl.multiple_of(k * mod_rows, 8), mod_rows)]

        def prepare():
            loads[5].wait()
            turn(raw_skip.at[0:width], w_skip.at[0], 0)
            turn(raw_skip.at[width : 2 * width], w_skip.at[1], 0)
            for copy in warm:
                copy.wait()
            for s in range(samples):
                hub[s, 0] = raw_warm[0, s].T
                hub[s, SLOTS] = raw_warm[1, s].T
                x_t[s, 0] = x_ref[s]
            w_in[...] = jnp.zeros_like(w_in)
            w_in[:, 0 : win_ref.shape[0]] = win_ref[...].T
            for half in range(2):
                spread(mods_at(0), half, mod_b.at[0])

        @pl.when(is_local)
        def _():
            arrived(mine(0), get_sem.at[0])
            prepare()
            for n in range(1, tail):
                arrived(mine(n), get_sem.at[n])

        @pl.when(jnp.logical_not(is_local))
        def _():
            for n in range(shared + 2):
                if n < shared:
                    arrived(mine(n, column), get_sem.at[n])
                    to_x(n).start()
                    to_y(n).start()
                if 1 <= n <= shared:
                    arrived(mine(n - 1, beside_x), put_sem.at[n - 1, 0])
                    on_y(n - 1).start()
                    arrived(mine(n - 1, beside_y), put_sem.at[n - 1, 1])
                    on_x(n - 1).start()
                if n >= 2:
                    arrived(mine(n - 2, across, 0), put_sem.at[n - 2, 2])
                    arrived(mine(n - 2, across, 1), put_sem.at[n - 2, 3])
                if n == 2:
                    prepare()
            for n in range(shared, tail):
                arrived(mine(n), get_sem.at[n])

        t = Scratch()
        t.qkv, t.o, t.act, t.s, t.p = s_qkv, s_o, s_act, s_s, s_p
        steps_a, steps_b = steps - 1 - pair, steps - pair
        count = jnp.where(first_half, steps_a, steps_b)
        chained = jnp.where(first_half, pair > 0, pair < last_pair)
        chains = jnp.where(first_half, pair < last_pair, pair > 0)
        chain_count = jnp.where(first_half, steps - 3 - pair, steps_b)

        def chain(k, s):
            slot = lax.rem(k + 1, SLOTS)
            return remote(outs.at[s, lax.rem(k, 2)], hub.at[s, slot], csend_sem.at[s, lax.rem(k, 2)], crecv_sem.at[s, slot], chain_to)

        def skip(k, s):
            slot = lax.rem(k + 1, SLOTS)
            return remote(outs.at[s, lax.rem(k, 2)], hub.at[s, SLOTS + slot], ssend_sem.at[s, lax.rem(k, 2)], srecv_sem.at[s, slot], peer)

        def latent(k, s):
            slot = lax.rem(k + 1, 2)
            return remote(x_t.at[s, slot], x_t.at[s, slot], xsend_sem.at[s, slot], xrecv_sem.at[s, slot], peer)

        def tell(n, s):
            return remote(x_end.at[s], x_end.at[s], esend_sem.at[s, n], erecv_sem.at[s], {"data": group, "stage": n})

        def step(m, _):
            k, s = m // samples, lax.rem(m, samples)
            slot, at = lax.rem(k, SLOTS), lax.rem(k, 2)

            @pl.when(m == HEAD // 2 * samples)
            def _():
                arrived(mine(tail), get_sem.at[tail])

            @pl.when(k > 1)
            def _():
                @pl.when(first_half)
                def _():
                    skip(k - 2, s).wait_send()

                @pl.when(chains)
                def _():
                    chain(k - 2, s).wait_send()

            @pl.when(jnp.logical_and(k > 0, chained))
            def _():
                arrived(hub.at[s, slot], crecv_sem.at[s, slot])

            @pl.when(jnp.logical_and(first_half, pair == 0))
            def _():
                @pl.when(k > 0)
                def _():
                    arrived(x_t.at[s, at], xrecv_sem.at[s, at])

                fill = jnp.zeros((CHUNK - channels, x_t.shape[3]), BF16)
                x_pad = jnp.concatenate([x_t[s, at].astype(BF16), fill], axis=0)
                for row in range(0, width, CHUNK):
                    h_ref[row : row + CHUNK] = product(w_in[row : row + CHUNK], x_pad)

            @pl.when(jnp.logical_and(first_half, pair > 0))
            def _():
                h_ref[...] = hub[s, slot].astype(F32)

            @pl.when(second_half)
            def _():
                @pl.when(k > 0)
                def _():
                    arrived(hub.at[s, SLOTS + slot], srecv_sem.at[s, slot])

                main = jnp.where(jnp.logical_and(k > 0, pair == last_pair), SLOTS + slot, slot)
                for row in range(0, width, CHUNK):
                    rows = slice(row, row + CHUNK)
                    h_ref[rows] = product(w_skip[1, rows], hub[s, SLOTS + slot]) + product(w_skip[0, rows], hub[s, main])

            block(
                h_ref, mod_b.at[at], all_w, outs.at[s, at], t, heads,
                lambda: spread(mods_at(jnp.minimum(k + 1, steps - 1)), s, mod_b.at[1 - at]),
            )

            @pl.when(jnp.logical_and(chains, k < chain_count))
            def _():
                @pl.when(k + 1 >= SLOTS)
                def _():
                    pl.semaphore_wait(ccredit_sem.at[s], 1)

                chain(k, s).start()

            @pl.when(first_half)
            def _():
                @pl.when(k + 1 >= SLOTS)
                def _():
                    pl.semaphore_wait(scredit_sem.at[s], 1)

                skip(k, s).start()

            @pl.when(jnp.logical_and(second_half, k + SLOTS < count))
            def _():
                pl.semaphore_signal(scredit_sem.at[s], inc=1, device_id=peer, device_id_type=mesh_ids)

            @pl.when(jnp.logical_and(chained, k + SLOTS < count))
            def _():
                pl.semaphore_signal(ccredit_sem.at[s], inc=1, device_id=chain_from, device_id_type=mesh_ids)

            @pl.when(jnp.logical_and(second_half, pair == 0))
            def _():
                @pl.when(k > 1)
                def _():
                    latent(k - 2, s).wait_send()

                noise = product(wout_ref[...], outs[s, at])
                x_new = keep_ref[k] * x_t[s, at] + noise_ref[k] * noise
                x_t[s, 1 - at] = x_new

                @pl.when(k < steps - 2)
                def _():
                    latent(k, s).start()

                @pl.when(k == steps - 1)
                def _():
                    x_end[s] = x_new
                    for n in range(stages):

                        @pl.when(n != me)
                        def _():
                            tell(n, s).start()

            return 0

        lax.fori_loop(0, count * samples, step, 0)

        for s in range(samples):
            for back in (2, 1):

                @pl.when(first_half)
                def _():
                    skip(count - back, s).wait_send()

                @pl.when(jnp.logical_and(second_half, chains))
                def _():
                    chain(count - back, s).wait_send()

        for n in range(n_parts):

            @pl.when(beside)
            def _():
                hand(n).wait_send()

            @pl.when(away)
            def _():
                leave(n).wait_send()

            if n < shared:

                @pl.when(jnp.logical_not(is_local))
                def _():
                    for copy in (to_x(n), to_y(n), on_y(n), on_x(n)):
                        copy.wait_send()

        holder = jnp.logical_and(second_half, pair == 0)
        for s in range(samples):

            @pl.when(holder)
            def _():
                for n in range(stages):

                    @pl.when(n != me)
                    def _():
                        tell(n, s).wait_send()

            @pl.when(jnp.logical_not(holder))
            def _():
                arrived(x_end.at[s], erecv_sem.at[s])

            out_ref[s] = x_end[s]

    def local_run(x_init, h_warm, skip_warm, w_in, w_out, w_qkv, w_o, w_up, w_down, w_skip, ada_mods, keep, noise):
        batch, tokens, channels = x_init.shape
        width, ff = w_up.shape[1], w_up.shape[2]
        heads = w_o.shape[1]
        steps = ada_mods.shape[0]
        rows = 4 * width + 2 * ff
        mod_rows = 6 * width // 128
        any_ = pl.BlockSpec(memory_space=pl.ANY)
        vmem = pl.BlockSpec(memory_space=pltpu.VMEM)
        smem = pl.BlockSpec(memory_space=pltpu.SMEM)
        V = pltpu.VMEM
        D = pltpu.SemaphoreType.DMA
        R = pltpu.SemaphoreType.REGULAR
        parts = len(PIECES) + 2
        scratch = [
            V((width, 3 * width), BF16), V((width, width), BF16), V((width, ff), BF16), V((ff, width), BF16),
            V((rows, width), BF16), V((steps * mod_rows, 128), F32), V((rows, width), BF16), V((steps * mod_rows, 128), F32),
            V((2 * width, width), BF16), V((2, width, width), BF16), V((2, batch, tokens, width), BF16), V((width, CHUNK), BF16),
            V((batch, 2 * SLOTS, width, tokens), BF16), V((batch, 2, width, tokens), BF16),
            V((batch, 2, channels, tokens), F32), V((batch, channels, tokens), F32), V((width, tokens), F32),
            V((3 * width, tokens), BF16), V((width, tokens), BF16), V((ff, tokens), BF16),
            V((AHEAD + 1, tokens, tokens), F32), V((2, tokens, tokens), BF16), V((2, 6, width, 128), F32),
            D((6,)), D((2,)), D((parts,)), D((parts,)), D((parts, 4)), D((parts, 4)),
            D((batch, 2)), D((batch, SLOTS)), D((batch, 2)), D((batch, SLOTS)), D((batch, 2)), D((batch, 2)),
            D((batch, stages)), D((batch,)), R((batch,)), R((batch,)),
        ]
        call = pl.pallas_call(
            functools.partial(kernel, steps, heads),
            out_shape=jax.ShapeDtypeStruct((batch, channels, tokens), F32),
            in_specs=[vmem, any_, any_, vmem, vmem, any_, any_, any_, any_, any_, any_, smem, smem],
            out_specs=vmem,
            scratch_shapes=scratch,
            compiler_params=pltpu.CompilerParams(collective_id=0, has_side_effects=True, vmem_limit_bytes=60 * 2**20),
            name="staged_sampler",
        )
        made = call(
            x_init.swapaxes(1, 2), h_warm, skip_warm, w_in, w_out.T, w_qkv, w_o.reshape(1, width, width), w_up, w_down,
            w_skip, ada_mods.reshape(steps * mod_rows, 128), keep, noise,
        )
        return made.swapaxes(1, 2)

    in_specs = (P('data'), P(None, 'data'), P(None, 'data'), P(), P(), P('stage'), P('stage'), P('stage'), P('stage'), P(), P(None, 'stage'), P(), P())
    return jax.shard_map(local_run, mesh=mesh, in_specs=in_specs, out_specs=P('data'), check_vma=False)
```
